32 devices in a mesh: lat: 8 (over y, x, core), lon: 4 (over z).
Axes of the slice: x: 2, y: 2, z: 4, core: 2. Of those that a mesh axis runs over, the one named last changes fastest.
Arguments:
- right_side: float32 [128, 2560], P('lat', 'lon'), may hold values from -34 to 34
- first_guess: float32 [128, 2560], P('lat', 'lon'), may hold values from -3 to 3
- cell_mask: int32 [128, 2560], P('lat', 'lon'), may hold values 0 or 1
- cond_east: float32 [128, 2560], P('lat', 'lon'), may hold values from 0.5 to 2
- cond_north: float32 [128, 2560], P('lat', 'lon'), may hold values from 0.5 to 2
- surface: float32 [128, 2560], P('lat', 'lon'), may hold values from 0.02 to 0.5
- recycled: float32 [16, 128, 2560], P(None, 'lat', 'lon'), may hold values from -0.0031444706 to 0.0031444706
Outputs:
- solution: float32 [128, 2560], P('lat', 'lon')
- residual: float32 [128, 2560], P('lat', 'lon')
The draws below stay inside these ranges and needn't reach their ends.
All inputs are finite; a program needn't handle non-finite values. No bound on the sum of `cell_mask` on one device may be relied on, other than what follows from the above.
Results may differ from the reference program's by a relative error of at most 0.0003.
Values sent between devices are 32-bit elements; how exact they have to be, the bound alone decides.
No kernel may reach another device: no remote copies, remote signals or barrier semaphores. Data moves between devices by JAX's collectives and lax.ppermute only.
A program may use at most 64 MiB of HBM per device.

```python
import math
import jax
import jax.numpy as jnp
from jax import lax

K = 16
ITERS = 3
NY = 128
NX = 2560


def basis_and_source(key):
    cells = NY * NX
    base = jax.random.fold_in(key, 7)
    key_phase, key_basis, key_weight, key_noise = jax.random.split(base, 4)
    phases = jax.random.uniform(key_phase, (2, K), jnp.float32, -3.1415927, 3.1415927)
    vector_index = jnp.arange(K)
    lat_wave = (vector_index % 4 + 1).astype(jnp.float32)
    lon_wave = (vector_index // 4 % 4).astype(jnp.float32)
    row_place = (jnp.arange(NY).astype(jnp.float32) + 0.5) / NY
    column_place = jnp.arange(NX).astype(jnp.float32) / NX
    lat_part = jnp.cos(3.1415927 * lat_wave[:, None] * row_place[None, :] + phases[0][:, None])
    lon_part = jnp.cos(6.2831853 * lon_wave[:, None] * column_place[None, :] + phases[1][:, None])
    pattern = lat_part[:, :, None] * lon_part[:, None, :]
    roughness = jnp.clip(jax.random.normal(key_basis, (K, NY, NX), jnp.float32), -4.0, 4.0)
    weights = jnp.clip(jax.random.normal(key_weight, (K,), jnp.float32), -2.5, 2.5) * 0.4
    noise = jnp.clip(jax.random.normal(key_noise, (NY, NX), jnp.float32), -4.0, 4.0)
    basis = pattern + 0.2 * roughness
    root = jnp.sqrt(jnp.float32(cells))
    source = noise + jnp.einsum('k,kyx->yx', weights, basis)
    return (basis / root, source)


def draw_recycled(key, part):
    return basis_and_source(key)[0].astype(jnp.float32)


def draw_right_side(key, part):
    return basis_and_source(key)[1].astype(jnp.float32)


def touch_ends(entries, own_key, low, high):
    longest = entries.shape.index(max(entries.shape))
    spots = []
    for shift in (0, 1):
        where = [jax.random.randint(jax.random.fold_in(own_key, axis), (), 0, length) for axis, length in enumerate(entries.shape)]
        where[longest] = (where[longest] + shift) % entries.shape[longest]
        spots.append(tuple(where))
    return entries.at[spots[0]].set(low).at[spots[1]].set(high)


def block_levels(rng, shape, cuts, low, top_value):
    gain = 1.0
    for axis_at, blocks in cuts:
        heights = jax.random.uniform(jax.random.fold_in(jax.random.fold_in(rng, 6), axis_at), (blocks,), jnp.float32, low / len(cuts), top_value / len(cuts))
        gain = gain * jnp.repeat(jnp.exp(heights), shape[axis_at] // blocks).reshape((-1,) + (1,) * (len(shape) - 1 - axis_at))
    return gain


def scatter_about(key, shape, width, bound, pieces=(), held_as=jnp.bfloat16):
    array = jax.random.normal(key, shape, jnp.float32) * width
    if len(pieces) > 0:
        array = block_levels(key, shape, pieces, -0.22, 0.18) * array
    return jnp.clip(array, min=-bound, max=bound).astype(held_as)


def setup_inputs(seed: int = 0) -> dict:
    key_of = jax.random.split(jax.random.key(seed), 8)
    right_side = draw_right_side(jax.random.fold_in(key_of[7], 71), 0)
    first_guess = scatter_about(key_of[1], (NY, NX), 0.5, 3.0, ((0, 8), (1, 4)), jnp.float32)
    cell_mask = touch_ends((jax.random.randint(key_of[2], (NY, NX), 0, 4) < 3).astype(jnp.int32), jax.random.fold_in(key_of[2], 1), 0, 1)
    cond_east = jnp.clip(jnp.exp(math.log(2.0) - 1.3862944 * jax.random.uniform(key_of[3], (NY, NX), jnp.float32) ** block_levels(key_of[3], (NY, NX), ((0, 8), (1, 4)), -0.2, 0.2)), 0.5, 2.0)
    cond_north = jnp.clip(jnp.exp(math.log(2.0) - 1.3862944 * jax.random.uniform(key_of[4], (NY, NX), jnp.float32) ** block_levels(key_of[4], (NY, NX), ((0, 8), (1, 4)), -0.2, 0.2)), 0.5, 2.0)
    surface = jnp.clip(jnp.exp(math.log(0.5) - 3.218876 * jax.random.uniform(key_of[5], (NY, NX), jnp.float32) ** block_levels(key_of[5], (NY, NX), ((0, 8), (1, 4)), -0.2, 0.2)), 0.02, 0.5)
    recycled = draw_recycled(jax.random.fold_in(key_of[7], 71), 0)
    return dict(right_side=right_side, first_guess=first_guess, cell_mask=cell_mask, cond_east=cond_east, cond_north=cond_north, surface=surface, recycled=recycled)


PRECISE = lax.Precision.HIGHEST

def neighbours(values):
    to_east = jnp.roll(values, -1, axis=-1)
    to_west = jnp.roll(values, 1, axis=-1)
    zero_row = jnp.zeros_like(values[..., :1, :])
    to_north = jnp.concatenate([values[..., 1:, :], zero_row], axis=-2)
    to_south = jnp.concatenate([zero_row, values[..., :-1, :]], axis=-2)
    return (to_east, to_west, to_north, to_south)

def faces(cell_mask, cond_east, cond_north, surface):
    wet_cells = cell_mask.astype(jnp.float32)
    wet_east = cond_east * wet_cells
    wet_north = cond_north * wet_cells
    ocean_e, ocean_w, ocean_n, ocean_s = neighbours(wet_cells)
    k_east = wet_east * ocean_e
    k_west = neighbours(wet_east)[1] * wet_cells
    k_north = wet_north * ocean_n
    k_south = neighbours(wet_north)[3] * wet_cells
    centre = surface * wet_cells + k_east + k_west + k_north + k_south + (1.0 - wet_cells)
    return (centre, k_east, k_west, k_north, k_south)

def operate(values, coeffs):
    centre, k_east, k_west, k_north, k_south = coeffs
    to_east, to_west, to_north, to_south = neighbours(values)
    return centre * values - (k_east * to_east + k_west * to_west + k_north * to_north + k_south * to_south)

def solve_small(factor, target):
    return jax.scipy.linalg.cho_solve((factor, True), target)

def reference(right_side, first_guess, cell_mask, cond_east, cond_north, surface, recycled):
    coeffs = faces(cell_mask, cond_east, cond_north, surface)
    basis_image = lax.map(lambda vector: operate(vector, coeffs), recycled)
    start_res = right_side - operate(first_guess, coeffs)
    gram = jnp.einsum('kyx,lyx->kl', recycled, basis_image, precision=PRECISE)
    start = jnp.einsum('kyx,yx->k', recycled, start_res, precision=PRECISE)
    factor = jnp.linalg.cholesky(0.5 * (gram + gram.T))
    coarse = solve_small(factor, start)
    solution = first_guess + jnp.einsum('kyx,k->yx', recycled, coarse, precision=PRECISE)
    residual = start_res - jnp.einsum('kyx,k->yx', basis_image, coarse, precision=PRECISE)
    direction = residual
    dir_image = residual
    curv = jnp.float32(1.0)
    prev_norm = jnp.float32(1.0)
    for turn_index in range(ITERS):
        image_res = operate(residual, coeffs)
        res_norm = jnp.sum(residual * residual)
        res_image = jnp.sum(residual * image_res)
        defl = jnp.einsum('kyx,yx->k', basis_image, residual, precision=PRECISE)
        coef = solve_small(factor, defl)
        along_basis = jnp.einsum('kyx,k->yx', recycled, coef, precision=PRECISE)
        along_image = jnp.einsum('kyx,k->yx', basis_image, coef, precision=PRECISE)
        if turn_index == 0:
            direction = residual - along_basis
            dir_image = image_res - along_image
            curv = res_image - jnp.sum(coef * defl)
        else:
            ratio = res_norm / prev_norm
            direction = residual - along_basis + ratio * direction
            dir_image = image_res - along_image + ratio * dir_image
            curv = res_image - jnp.sum(coef * defl) - ratio * ratio * curv
        step_len = res_norm / curv
        solution = solution + step_len * direction
        residual = residual - step_len * dir_image
        prev_norm = res_norm
    return (solution, residual)
```

```python
import functools

import jax
import jax.numpy as jnp
from jax import lax
from jax.experimental import pallas as pl
from jax.experimental.pallas import tpu as pltpu
from jax.sharding import PartitionSpec as P

SHIFT = 5.0
ITERS = 3
DEPTH = ITERS + 1
LANES = 128


def ring(count, step):
    return [(i, (i + step) % count) for i in range(count)]


def pack_kernel(basis, guess, rhs, mask, east, north, surf, to_n, to_s, to_e, to_w):
    vectors, rows, cols = basis.shape
    fields = [basis.at[k] for k in range(vectors)] + [guess, rhs, mask, east, north, surf]
    strip_e = jnp.zeros((rows, LANES), jnp.float32)
    strip_w = jnp.zeros((rows, LANES), jnp.float32)
    lane = lax.broadcasted_iota(jnp.int32, (rows, LANES), 1)
    for f, ref in enumerate(fields):
        at = DEPTH * f
        to_n[pl.ds(at, DEPTH), :] = ref[rows - DEPTH :, :].astype(jnp.float32)
        to_s[pl.ds(at, DEPTH), :] = ref[:DEPTH, :].astype(jnp.float32)
        here = (lane >= at) & (lane < at + DEPTH)
        last = ref[:, cols - LANES :].astype(jnp.float32)
        first = ref[:, :LANES].astype(jnp.float32)
        strip_e = jnp.where(here, pltpu.roll(last, (at + DEPTH) % LANES, 1), strip_e)
        strip_w = jnp.where(here, pltpu.roll(first, at, 1), strip_w)
    to_e[...] = strip_e
    to_w[...] = strip_w


def roll_lanes(v, by):
    return pltpu.roll(v, by % v.shape[1], 1)


def roll_rows(v, by):
    return pltpu.roll(v, by % v.shape[0], 0)


def apply_faces(v, diag, k_east, k_north):
    flux_e = k_east * (v - roll_lanes(v, -1))
    flux_n = k_north * (v - roll_rows(v, -1))
    return diag * v + (flux_e - roll_lanes(flux_e, 1)) + (flux_n - roll_rows(flux_n, 1))


def moments_kernel(
    place, basis, guess, rhs, mask, east, north, surf,
    from_n, from_s, from_e, from_w, ne, nw, se, sw,
    copies, basis_ext, side_ext, powers, fields_ext,
):
    vectors, rows, cols = basis.shape
    wide = cols + LANES
    tall = rows + 2 * DEPTH
    lane = lax.broadcasted_iota(jnp.int32, (tall, LANES), 1)
    strip_e = jnp.concatenate([from_e[...], ne[:DEPTH, :], se[rows - DEPTH :, :]], axis=0)
    strip_w = jnp.concatenate([from_w[...], nw[:DEPTH, :], sw[rows - DEPTH :, :]], axis=0)

    def extend(f, own, out):
        at = DEPTH * f
        out[:rows, :cols] = own.astype(jnp.float32)
        out[rows : rows + DEPTH, :cols] = from_n[pl.ds(at, DEPTH), :]
        out[rows + DEPTH :, :cols] = from_s[pl.ds(at, DEPTH), :]
        edge_e = pltpu.roll(strip_e, (-at) % LANES, 1)
        edge_w = pltpu.roll(strip_w, (LANES - DEPTH - at) % LANES, 1)
        edge = jnp.where(lane < DEPTH, edge_e, jnp.where(lane >= LANES - DEPTH, edge_w, 0.0))
        out[:, cols:] = edge

    for k in range(vectors):
        extend(k, basis[k], basis_ext.at[k])
    for f, ref in enumerate((guess, rhs, mask, east, north, surf)):
        extend(vectors + f, ref[...], fields_ext.at[f])
    row = lax.broadcasted_iota(jnp.int32, (tall, wide), 0)
    beyond_n = (row >= rows) & (row < rows + DEPTH) & (place[0] == place[1] - 1)
    beyond_s = (row >= rows + DEPTH) & (place[0] == 0)
    wet = jnp.where(beyond_n | beyond_s, 0.0, fields_ext[2])
    k_east = fields_ext[3] * wet * roll_lanes(wet, -1)
    k_north = fields_ext[4] * wet * roll_rows(wet, -1)
    diag = fields_ext[5] * wet + (1.0 - wet)
    side_ext[0] = diag
    side_ext[1] = k_east
    side_ext[2] = k_north
    start = fields_ext[1] - apply_faces(fields_ext[0], diag, k_east, k_north)
    side_ext[3] = start

    def put(index, v):
        for tile in range(cols // LANES):
            at = tile * LANES
            powers[tile, pl.ds(index * rows, rows), :] = v[:rows, at : at + LANES]

    def shifted(v):
        return apply_faces(v, side_ext[0] - SHIFT, side_ext[1], side_ext[2])

    def one_vector(k, carry):
        v = basis_ext[k]
        put(k, v)
        v = apply_faces(v, side_ext[0], side_ext[1], side_ext[2])
        put(vectors + k, v)
        for power in range(ITERS):
            v = shifted(v)
            put((2 + power) * vectors + k, v)
        return carry

    lax.fori_loop(0, vectors, one_vector, 0)
    v = start
    base = (ITERS + 2) * vectors
    put(base, v)
    for power in range(ITERS):
        v = shifted(v)
        put(base + 1 + power, v)
    spare = 8 - (ITERS + 1)
    powers[:, pl.ds((base + ITERS + 1) * rows, spare * rows), :] = jnp.zeros(
        (cols // LANES, spare * rows, LANES), jnp.float32
    )
    count = base + 8
    nt = (((1,), (1,)), ((), ()))

    def one_row(r, carry):
        high_sum, cross_sum = carry
        tiles = range(cols // LANES)
        x = [powers[tile, pl.ds(r, count, stride=rows), :] for tile in tiles]
        x = jnp.concatenate(x, axis=1)
        high = x.astype(jnp.bfloat16)
        low = (x - high.astype(jnp.float32)).astype(jnp.bfloat16)
        high_sum += lax.dot_general(high, high, nt, preferred_element_type=jnp.float32)
        cross_sum += lax.dot_general(high, low, nt, preferred_element_type=jnp.float32)
        return high_sum, cross_sum

    zero = jnp.zeros((count, count), jnp.float32)
    high_sum, cross_sum = lax.fori_loop(0, rows, one_row, (zero, zero))
    full = high_sum + cross_sum + cross_sum.T
    full = jnp.concatenate([full, jnp.zeros((count, LANES - count), jnp.float32)], axis=1)
    at = lax.broadcasted_iota(jnp.int32, (vectors, LANES), 1)
    slabs = [full[a * vectors : (a + 1) * vectors, :] for a in range(4)]
    tail = jnp.concatenate([full[base:, :], jnp.zeros((vectors - 8, LANES), jnp.float32)], axis=0)
    out = jnp.zeros((vectors, LANES), jnp.float32)

    def move(out, v, first, width, target):
        moved = pltpu.roll(v, (target - first) % LANES, 1)
        return jnp.where((at >= target) & (at < target + width), moved, out)

    out = move(out, slabs[0], vectors, vectors, 0)
    out = move(out, slabs[1], vectors, 2 * vectors, vectors)
    out = move(out, slabs[2], 2 * vectors, 2 * vectors, 3 * vectors)
    out = move(out, slabs[3], 3 * vectors, 2 * vectors, 5 * vectors)
    free = 7 * vectors
    out = move(out, slabs[0], base, 1, free)
    out = move(out, slabs[1], base, 2, free + 1)
    out = move(out, slabs[2], base + 1, 2, free + 3)
    out = move(out, slabs[3], base + 2, 2, free + 5)
    out = move(out, tail, base, 4, free + 8)

    def one_copy(device, carry):
        copies[device] = out
        return carry

    lax.fori_loop(0, copies.shape[0], one_copy, 0, unroll=8)


def finish_kernel(parts, guess, basis_ext, side_ext, solution, residual, spread):
    vectors, tall, wide = basis_ext.shape
    rows, cols = guess.shape
    free = 7 * vectors
    several = 8

    def add_parts(i, sums):
        return tuple(sums[n] + parts[i * several + n] for n in range(several))

    nothing = (jnp.zeros(parts.shape[1:], jnp.float32),) * several
    sums = list(lax.fori_loop(0, parts.shape[0] // several, add_parts, nothing, unroll=2))
    while len(sums) > 1:
        sums = [sums[i] + sums[i + 1] for i in range(0, len(sums), 2)]
    total = sums[0]
    lane = lax.broadcasted_iota(jnp.int32, (vectors, LANES), 1)
    sub = lax.broadcasted_iota(jnp.int32, (vectors, LANES), 0)
    table = total
    for i in range(vectors):
        column = table[:, i : i + 1]
        pivot_row = table[i : i + 1, :] / table[i : i + 1, i : i + 1]
        table = jnp.where(sub == i, pivot_row, table - column * pivot_row)
    own_lane = (lane % vectors) == sub
    z = [-table[:, free : free + 1]]
    sums = jnp.zeros((vectors, LANES), jnp.float32)
    history = jnp.zeros((1, LANES), jnp.float32)
    lane_row = lane[:1, :]
    for j in range(2 * ITERS):
        newest = jnp.sum(jnp.where(own_lane, z[j], 0.0), axis=0, keepdims=True)
        history = pltpu.roll(history, vectors, 1)
        history = jnp.where((lane_row >= vectors) & (lane_row < 2 * vectors), newest, history)
        terms = (lane >= vectors) & (lane < (j + 2) * vectors)
        weights = jnp.where(terms, history, jnp.where(lane == free + 1 + j, 1.0, 0.0))
        z.append(-jnp.sum(table * weights, axis=1, keepdims=True))
    for j in range(2 * ITERS + 1):
        sums = sums + pltpu.roll(jnp.where(lane >= free, total, 0.0) * z[j], j, 1)
    picked = jnp.where((lane > free) & (lane < free + 7), sums, 0.0)
    for a in range(ITERS):
        moved = pltpu.roll(total, (a - 7) % LANES, 1)
        first = free + 1 + 2 * a
        picked += jnp.where((sub == a) & (lane >= first) & (lane < first + 2), moved, 0.0)
    moment_row = jnp.sum(picked, axis=0, keepdims=True)
    mu = [moment_row[:, free + 1 + k : free + 2 + k] for k in range(2 * ITERS)]
    for i in range(ITERS + 1):
        spread[i] = jnp.broadcast_to(z[i], (vectors, LANES))

    nil = jnp.zeros((1, 1), jnp.float32)
    rho = [nil + 1.0] + [nil] * ITERS
    gamma = [nil] * (ITERS + 1)
    delta = [nil] * ITERS
    curv = nil
    prev = nil
    for j in range(ITERS):
        norm = nil
        image = nil
        for a in range(j + 1):
            for b in range(j + 1):
                pair = rho[a] * rho[b]
                norm += pair * mu[a + b]
                image += pair * (mu[a + b + 1] + SHIFT * mu[a + b])
        if j == 0:
            gamma = list(rho)
            curv = image
        else:
            ratio = norm / prev
            gamma = [rho[i] + ratio * gamma[i] for i in range(ITERS + 1)]
            curv = image - ratio * ratio * curv
        step = norm / curv
        delta = [delta[i] + step * gamma[i] for i in range(ITERS)]
        below = [nil] + gamma[:ITERS]
        rho = [rho[i] - step * (SHIFT * gamma[i] + below[i]) for i in range(ITERS + 1)]
        prev = norm

    along = [[] for _ in range(ITERS + 1)]
    for tile in range(wide // LANES):
        acc = [jnp.zeros((tall, LANES), jnp.float32) for _ in range(ITERS + 1)]
        for k in range(vectors):
            w = basis_ext[k, :, pl.ds(tile * LANES, LANES)]
            for i in range(ITERS + 1):
                acc[i] = acc[i] + w * spread[i, pl.ds(k, 1), :]
        for i in range(ITERS + 1):
            along[i].append(acc[i])
    along = [jnp.concatenate(pieces, axis=1) for pieces in along]
    diag, k_east, k_north = side_ext[0], side_ext[1], side_ext[2]
    image = functools.partial(apply_faces, k_east=k_east, k_north=k_north)
    v = side_ext[3] + image(along[0], diag)
    x = guess[...] - along[0][:rows, :cols]
    r = rho[0] * v[:rows, :cols]
    for i in range(ITERS):
        x = x + delta[i] * (v + along[i + 1])[:rows, :cols]
        v = image(v, diag - SHIFT) + image(along[i + 1], diag)
        r = r + rho[i + 1] * v[:rows, :cols]
    solution[...] = x
    residual[...] = r


def call(kernel, out_shape, inputs, scratch=(), smem=0, name=None):
    specs = [pl.BlockSpec(memory_space=pltpu.SMEM)] * smem
    specs += [pl.BlockSpec(memory_space=pltpu.VMEM)] * (len(inputs) - smem)
    return pl.pallas_call(
        kernel,
        out_shape=out_shape,
        in_specs=specs,
        out_specs=[pl.BlockSpec(memory_space=pltpu.VMEM)] * len(out_shape),
        scratch_shapes=scratch,
        name=name,
        compiler_params=pltpu.CompilerParams(vmem_limit_bytes=24 * 1024 * 1024),
    )(*inputs)


def f32(*shape):
    return jax.ShapeDtypeStruct(shape, jnp.float32)


def shards(right_side, first_guess, cell_mask, cond_east, cond_north, surface, recycled):
    vectors, rows, cols = recycled.shape
    n_lat, n_lon = lax.axis_size("lat"), lax.axis_size("lon")
    devices = n_lat * n_lon
    fields = vectors + 6
    tall, wide = rows + 2 * DEPTH, cols + LANES
    own = (recycled, first_guess, right_side, cell_mask, cond_east, cond_north, surface)
    band, strip = f32(fields * DEPTH, cols), f32(rows, LANES)
    to_n, to_s, to_e, to_w = call(pack_kernel, [band, band, strip, strip], own, name="pack")
    north, south = ring(n_lat, 1), ring(n_lat, -1)
    from_w = lax.ppermute(to_e, "lon", ring(n_lon, 1))
    from_e = lax.ppermute(to_w, "lon", ring(n_lon, -1))
    from_s = lax.ppermute(to_n, "lat", north)
    from_n = lax.ppermute(to_s, "lat", south)
    se, sw = lax.ppermute(from_e, "lat", north), lax.ppermute(from_w, "lat", north)
    ne, nw = lax.ppermute(from_e, "lat", south), lax.ppermute(from_w, "lat", south)
    place = jnp.stack([lax.axis_index("lat"), jnp.int32(n_lat)])
    copies, basis_ext, side_ext = call(
        moments_kernel,
        [f32(devices, vectors, LANES), f32(vectors, tall, wide), f32(4, tall, wide)],
        (place,) + own + (from_n, from_s, from_e, from_w, ne, nw, se, sw),
        scratch=[
            pltpu.VMEM((cols // LANES, ((ITERS + 2) * vectors + 8) * rows, LANES), jnp.float32),
            pltpu.VMEM((6, tall, wide), jnp.float32),
        ],
        smem=1,
        name="moments",
    )
    parts = lax.all_to_all(copies, ("lat", "lon"), 0, 0)
    return call(
        finish_kernel,
        [f32(rows, cols), f32(rows, cols)],
        (parts, first_guess, basis_ext, side_ext),
        scratch=[pltpu.VMEM((ITERS + 1, vectors, LANES), jnp.float32)],
        name="finish",
    )


def solution(mesh):
    block = P("lat", "lon")
    return jax.shard_map(
        shards,
        mesh=mesh,
        in_specs=(block,) * 6 + (P(None, "lat", "lon"),),
        out_specs=(block, block),
        check_vma=False,
    )
```

```python
import functools

import jax
import jax.numpy as jnp
from jax import lax
from jax.experimental import pallas as pl
from jax.experimental.pallas import tpu as pltpu
from jax.sharding import PartitionSpec as P

SHIFT = 5.0
ITERS = 3
DEPTH = ITERS + 1
LANES = 128


def ring(count, step):
    return [(i, (i + step) % count) for i in range(count)]


def pack_kernel(
    basis_hbm, guess_hbm, rhs_hbm, mask_hbm, east_hbm, north_hbm, surf_hbm,
    basis, sides, mask, to_n, to_s, to_e, to_w, sems,
):
    vectors, rows, cols = basis.shape
    moves = [(basis_hbm, basis), (mask_hbm, mask)]
    sources = (guess_hbm, rhs_hbm, east_hbm, north_hbm, surf_hbm)
    moves += [(source, sides.at[i]) for i, source in enumerate(sources)]
    copies = [pltpu.make_async_copy(a, b, sems.at[i]) for i, (a, b) in enumerate(moves)]
    for copy in copies:
        copy.start()
    for copy in copies:
        copy.wait()
    fields = [basis.at[k] for k in range(vectors)]
    fields += [sides.at[0], sides.at[1], mask, sides.at[2], sides.at[3], sides.at[4]]
    strip_e = jnp.zeros((rows, LANES), jnp.float32)
    strip_w = jnp.zeros((rows, LANES), jnp.float32)
    lane = lax.broadcasted_iota(jnp.int32, (rows, LANES), 1)
    for f, ref in enumerate(fields):
        at = DEPTH * f
        to_n[pl.ds(at, DEPTH), :] = ref[rows - DEPTH :, :].astype(jnp.float32)
        to_s[pl.ds(at, DEPTH), :] = ref[:DEPTH, :].astype(jnp.float32)
        here = (lane >= at) & (lane < at + DEPTH)
        last = ref[:, cols - LANES :].astype(jnp.float32)
        first = ref[:, :LANES].astype(jnp.float32)
        strip_e = jnp.where(here, pltpu.roll(last, (at + DEPTH) % LANES, 1), strip_e)
        strip_w = jnp.where(here, pltpu.roll(first, at, 1), strip_w)
    to_e[...] = strip_e
    to_w[...] = strip_w


def roll_lanes(v, by):
    return pltpu.roll(v, by % v.shape[1], 1)


def roll_rows(v, by):
    return pltpu.roll(v, by % v.shape[0], 0)


def apply_faces(v, diag, k_east, k_north):
    flux_e = k_east * (v - roll_lanes(v, -1))
    flux_n = k_north * (v - roll_rows(v, -1))
    return diag * v + (flux_e - roll_lanes(flux_e, 1)) + (flux_n - roll_rows(flux_n, 1))


def moments_kernel(
    place, basis, sides, mask,
    from_n, from_s, from_e, from_w, corner_n, corner_s,
    copies, basis_ext, side_ext, powers, fields_ext, faces, start_powers,
):
    vectors, rows, cols = basis.shape
    wide = cols + LANES
    tall = rows + 2 * DEPTH
    tiles = cols // LANES
    lane = lax.broadcasted_iota(jnp.int32, (tall, LANES), 1)
    strip_e = [from_e[...], corner_n[:DEPTH, :], corner_s[rows - DEPTH : rows, :]]
    strip_w = [from_w[...], corner_n[rows : rows + DEPTH, :], corner_s[2 * rows - DEPTH :, :]]
    strip_e = jnp.concatenate(strip_e, axis=0)
    strip_w = jnp.concatenate(strip_w, axis=0)

    def edge_of(f):
        at = DEPTH * f
        edge_e = pltpu.roll(strip_e, (-at) % LANES, 1)
        edge_w = pltpu.roll(strip_w, (LANES - DEPTH - at) % LANES, 1)
        return jnp.where(lane < DEPTH, edge_e, jnp.where(lane >= LANES - DEPTH, edge_w, 0.0))

    for k in range(vectors):
        at, to = DEPTH * k, tall * k
        for tile in range(tiles):
            part = pl.ds(tile * LANES, LANES)
            basis_ext[tile, pl.ds(to, rows), :] = basis[k, :, part]
            basis_ext[tile, pl.ds(to + rows, DEPTH), :] = from_n[pl.ds(at, DEPTH), part]
            basis_ext[tile, pl.ds(to + rows + DEPTH, DEPTH), :] = from_s[pl.ds(at, DEPTH), part]
        basis_ext[tiles, pl.ds(to, tall), :] = edge_of(k)
    own = (sides.at[0], sides.at[1], mask, sides.at[2], sides.at[3], sides.at[4])
    for f, ref in enumerate(own):
        at = DEPTH * (vectors + f)
        fields_ext[f, :rows, :cols] = ref[...].astype(jnp.float32)
        fields_ext[f, rows : rows + DEPTH, :cols] = from_n[pl.ds(at, DEPTH), :]
        fields_ext[f, rows + DEPTH :, :cols] = from_s[pl.ds(at, DEPTH), :]
        fields_ext[f, :, cols:] = edge_of(vectors + f)
    row = lax.broadcasted_iota(jnp.int32, (tall, wide), 0)
    beyond_n = (row >= rows) & (row < rows + DEPTH) & (place[0] == place[1] - 1)
    beyond_s = (row >= rows + DEPTH) & (place[0] == 0)
    wet = jnp.where(beyond_n | beyond_s, 0.0, fields_ext[2])
    k_east = fields_ext[3] * wet * roll_lanes(wet, -1)
    k_north = fields_ext[4] * wet * roll_rows(wet, -1)
    diag = fields_ext[5] * wet + (1.0 - wet)
    side_ext[0] = diag
    side_ext[1] = k_east
    side_ext[2] = k_north
    start = fields_ext[1] - apply_faces(fields_ext[0], diag, k_east, k_north)
    side_ext[3] = start
    v = start
    for power in range(ITERS + 1):
        for tile in range(tiles):
            part = v[:rows, tile * LANES : (tile + 1) * LANES]
            start_powers[tile, pl.ds(power * rows, rows), :] = part
        if power < ITERS:
            v = apply_faces(v, side_ext[0] - SHIFT, side_ext[1], side_ext[2])
    spare = (8 - (ITERS + 1)) * rows
    start_powers[:, pl.ds((ITERS + 1) * rows, spare), :] = jnp.zeros(
        (tiles, spare, LANES), jnp.float32
    )

    for q in range(tall):
        ring_row = (q - DEPTH) % tall
        for c, coeff in enumerate((side_ext.at[0], side_ext.at[1], side_ext.at[2])):
            spread = jnp.broadcast_to(coeff[ring_row : ring_row + 1, :], (8, wide))
            faces[c, q] = spread
            if c == 0:
                faces[3, q] = spread - SHIFT
        for tile in range(tiles + 1):
            part = basis_ext[tile, pl.ds(ring_row, vectors, stride=tall), :]
            powers[q, :vectors, tile * LANES : (tile + 1) * LANES] = part

    def coefficient(c, q):
        return jnp.concatenate([faces[c, q]] * (vectors // 8), axis=0)

    unroll = 2
    for power in range(DEPTH):
        first, last = 1 + power, tall - 1 - power
        source = slice(power * vectors, (power + 1) * vectors)
        target = slice((power + 1) * vectors, (power + 2) * vectors)
        middle = 0 if power == 0 else 3

        def some_rows(i, flux_s, first=first, source=source, target=target, middle=middle):
            for u in range(unroll):
                q = first + i * unroll + u
                v = powers[q, source, :]
                flux_n = coefficient(2, q) * (v - powers[q + 1, source, :])
                flux_e = coefficient(1, q) * (v - roll_lanes(v, -1))
                image = coefficient(middle, q) * v + (flux_e - roll_lanes(flux_e, 1))
                powers[q, target, :] = image + (flux_n - flux_s)
                flux_s = flux_n
            return flux_s

        below = first - 1
        flux = powers[below, source, :] - powers[first, source, :]
        lax.fori_loop(0, (last - first) // unroll, some_rows, coefficient(2, below) * flux)

    base = (ITERS + 2) * vectors
    count = base + 8
    batch = 4
    nt = (((1,), (1,)), ((), ()))

    def one_batch(i, carry):
        high_sum, cross_sum = carry
        x = []
        for u in range(batch):
            r = i * batch + u
            tail = [start_powers[t, pl.ds(r, 8, stride=rows), :] for t in range(tiles)]
            tail = jnp.concatenate(tail, axis=1)
            x.append(jnp.concatenate([powers[r + DEPTH, :, :cols], tail], axis=0))
        x = jnp.concatenate(x, axis=1)
        high = x.astype(jnp.bfloat16)
        low = (x - high.astype(jnp.float32)).astype(jnp.bfloat16)
        high_sum += lax.dot_general(high, high, nt, preferred_element_type=jnp.float32)
        cross_sum += lax.dot_general(high, low, nt, preferred_element_type=jnp.float32)
        return high_sum, cross_sum

    zero = jnp.zeros((count, count), jnp.float32)
    high_sum, cross_sum = lax.fori_loop(0, rows // batch, one_batch, (zero, zero))
    full = high_sum + cross_sum + cross_sum.T
    full = jnp.concatenate([full, jnp.zeros((count, LANES - count), jnp.float32)], axis=1)
    at = lax.broadcasted_iota(jnp.int32, (vectors, LANES), 1)
    slabs = [full[a * vectors : (a + 1) * vectors, :] for a in range(4)]
    tail = jnp.concatenate([full[base:, :], jnp.zeros((vectors - 8, LANES), jnp.float32)], axis=0)
    out = jnp.zeros((vectors, LANES), jnp.float32)

    def move(out, v, first, width, target):
        moved = pltpu.roll(v, (target - first) % LANES, 1)
        return jnp.where((at >= target) & (at < target + width), moved, out)

    out = move(out, slabs[0], vectors, vectors, 0)
    out = move(out, slabs[1], vectors, 2 * vectors, vectors)
    out = move(out, slabs[2], 2 * vectors, 2 * vectors, 3 * vectors)
    out = move(out, slabs[3], 3 * vectors, 2 * vectors, 5 * vectors)
    free = 7 * vectors
    out = move(out, slabs[0], base, 1, free)
    out = move(out, slabs[1], base, 2, free + 1)
    out = move(out, slabs[2], base + 1, 2, free + 3)
    out = move(out, slabs[3], base + 2, 2, free + 5)
    out = move(out, tail, base, 4, free + 8)

    def one_copy(device, carry):
        copies[device] = out
        return carry

    lax.fori_loop(0, copies.shape[0], one_copy, 0, unroll=8)


def finish_kernel(parts, sides, basis_ext, side_ext, solution, residual, spread):
    _, tall, wide = side_ext.shape
    _, rows, cols = sides.shape
    vectors = basis_ext.shape[1] // tall
    free = 7 * vectors
    several = 8

    def add_parts(i, sums):
        return tuple(sums[n] + parts[i * several + n] for n in range(several))

    nothing = (jnp.zeros(parts.shape[1:], jnp.float32),) * several
    sums = list(lax.fori_loop(0, parts.shape[0] // several, add_parts, nothing, unroll=2))
    while len(sums) > 1:
        sums = [sums[i] + sums[i + 1] for i in range(0, len(sums), 2)]
    total = sums[0]
    lane = lax.broadcasted_iota(jnp.int32, (vectors, LANES), 1)
    sub = lax.broadcasted_iota(jnp.int32, (vectors, LANES), 0)
    table = total
    for i in range(vectors):
        column = table[:, i : i + 1]
        pivot_row = table[i : i + 1, :] / table[i : i + 1, i : i + 1]
        table = jnp.where(sub == i, pivot_row, table - column * pivot_row)
    own_lane = (lane % vectors) == sub
    z = [-table[:, free : free + 1]]
    sums = jnp.zeros((vectors, LANES), jnp.float32)
    history = jnp.zeros((1, LANES), jnp.float32)
    lane_row = lane[:1, :]
    for j in range(2 * ITERS):
        newest = jnp.sum(jnp.where(own_lane, z[j], 0.0), axis=0, keepdims=True)
        history = pltpu.roll(history, vectors, 1)
        history = jnp.where((lane_row >= vectors) & (lane_row < 2 * vectors), newest, history)
        terms = (lane >= vectors) & (lane < (j + 2) * vectors)
        weights = jnp.where(terms, history, jnp.where(lane == free + 1 + j, 1.0, 0.0))
        z.append(-jnp.sum(table * weights, axis=1, keepdims=True))
    for j in range(2 * ITERS + 1):
        sums = sums + pltpu.roll(jnp.where(lane >= free, total, 0.0) * z[j], j, 1)
    picked = jnp.where((lane > free) & (lane < free + 7), sums, 0.0)
    for a in range(ITERS):
        moved = pltpu.roll(total, (a - 7) % LANES, 1)
        first = free + 1 + 2 * a
        picked += jnp.where((sub == a) & (lane >= first) & (lane < first + 2), moved, 0.0)
    moment_row = jnp.sum(picked, axis=0, keepdims=True)
    mu = [moment_row[:, free + 1 + k : free + 2 + k] for k in range(2 * ITERS)]
    for i in range(ITERS + 1):
        spread[i] = jnp.broadcast_to(z[i], (vectors, LANES))

    nil = jnp.zeros((1, 1), jnp.float32)
    rho = [nil + 1.0] + [nil] * ITERS
    gamma = [nil] * (ITERS + 1)
    delta = [nil] * ITERS
    curv = nil
    prev = nil
    for j in range(ITERS):
        norm = nil
        image = nil
        for a in range(j + 1):
            for b in range(j + 1):
                pair = rho[a] * rho[b]
                norm += pair * mu[a + b]
                image += pair * (mu[a + b + 1] + SHIFT * mu[a + b])
        if j == 0:
            gamma = list(rho)
            curv = image
        else:
            ratio = norm / prev
            gamma = [rho[i] + ratio * gamma[i] for i in range(ITERS + 1)]
            curv = image - ratio * ratio * curv
        step = norm / curv
        delta = [delta[i] + step * gamma[i] for i in range(ITERS)]
        below = [nil] + gamma[:ITERS]
        rho = [rho[i] - step * (SHIFT * gamma[i] + below[i]) for i in range(ITERS + 1)]
        prev = norm

    along = [[] for _ in range(ITERS + 1)]
    for tile in range(wide // LANES):
        acc = [jnp.zeros((tall, LANES), jnp.float32) for _ in range(ITERS + 1)]
        for k in range(vectors):
            w = basis_ext[tile, pl.ds(tall * k, tall), :]
            for i in range(ITERS + 1):
                acc[i] = acc[i] + w * spread[i, pl.ds(k, 1), :]
        for i in range(ITERS + 1):
            along[i].append(acc[i])
    along = [jnp.concatenate(pieces, axis=1) for pieces in along]
    diag, k_east, k_north = side_ext[0], side_ext[1], side_ext[2]
    image = functools.partial(apply_faces, k_east=k_east, k_north=k_north)
    v = side_ext[3] + image(along[0], diag)
    x = sides[0] - along[0][:rows, :cols]
    r = rho[0] * v[:rows, :cols]
    for i in range(ITERS):
        x = x + delta[i] * (v + along[i + 1])[:rows, :cols]
        v = image(v, diag - SHIFT) + image(along[i + 1], diag)
        r = r + rho[i + 1] * v[:rows, :cols]
    solution[...] = x
    residual[...] = r


def call(kernel, out_shape, spaces, inputs, scratch=(), name=None):
    return pl.pallas_call(
        kernel,
        out_shape=out_shape,
        in_specs=[pl.BlockSpec(memory_space=space) for space in spaces],
        out_specs=[pl.BlockSpec(memory_space=pltpu.VMEM)] * len(out_shape),
        scratch_shapes=scratch,
        name=name,
        compiler_params=pltpu.CompilerParams(vmem_limit_bytes=24 * 1024 * 1024),
    )(*inputs)


def f32(*shape):
    return jax.ShapeDtypeStruct(shape, jnp.float32)


def shards(right_side, first_guess, cell_mask, cond_east, cond_north, surface, recycled):
    vectors, rows, cols = recycled.shape
    n_lat, n_lon = lax.axis_size("lat"), lax.axis_size("lon")
    devices = n_lat * n_lon
    fields = vectors + 6
    tall, wide = rows + 2 * DEPTH, cols + LANES
    tiles = cols // LANES
    own = (recycled, first_guess, right_side, cell_mask, cond_east, cond_north, surface)
    band, strip = f32(fields * DEPTH, cols), f32(rows, LANES)
    basis, sides, mask, to_n, to_s, to_e, to_w = call(
        pack_kernel,
        [f32(vectors, rows, cols), f32(5, rows, cols), jax.ShapeDtypeStruct((rows, cols), jnp.int32)]
        + [band, band, strip, strip],
        [pltpu.HBM] * 7,
        own,
        scratch=[pltpu.SemaphoreType.DMA((7,))],
        name="pack",
    )
    north, south = ring(n_lat, 1), ring(n_lat, -1)
    from_w = lax.ppermute(to_e, "lon", ring(n_lon, 1))
    from_e = lax.ppermute(to_w, "lon", ring(n_lon, -1))
    from_s = lax.ppermute(to_n, "lat", north)
    from_n = lax.ppermute(to_s, "lat", south)
    strips = jnp.concatenate([from_e, from_w], axis=0)
    corner_s = lax.ppermute(strips, "lat", north)
    corner_n = lax.ppermute(strips, "lat", south)
    place = jnp.stack([lax.axis_index("lat"), jnp.int32(n_lat)])
    copies, basis_ext, side_ext = call(
        moments_kernel,
        [f32(devices, vectors, LANES), f32(tiles + 1, vectors * tall, LANES), f32(4, tall, wide)],
        [pltpu.SMEM] + [pltpu.VMEM] * 9,
        (place, basis, sides, mask, from_n, from_s, from_e, from_w, corner_n, corner_s),
        scratch=[
            pltpu.VMEM((tall, (ITERS + 2) * vectors, wide), jnp.float32),
            pltpu.VMEM((6, tall, wide), jnp.float32),
            pltpu.VMEM((4, tall, 8, wide), jnp.float32),
            pltpu.VMEM((tiles, 8 * rows, LANES), jnp.float32),
        ],
        name="moments",
    )
    parts = lax.all_to_all(copies, ("lat", "lon"), 0, 0)
    return call(
        finish_kernel,
        [f32(rows, cols), f32(rows, cols)],
        [pltpu.VMEM] * 4,
        (parts, sides, basis_ext, side_ext),
        scratch=[pltpu.VMEM((ITERS + 1, vectors, LANES), jnp.float32)],
        name="finish",
    )


def solution(mesh):
    block = P("lat", "lon")
    return jax.shard_map(
        shards,
        mesh=mesh,
        in_specs=(block,) * 6 + (P(None, "lat", "lon"),),
        out_specs=(block, block),
        check_vma=False,
    )
```

```python
import functools

import jax
import jax.numpy as jnp
from jax import lax
from jax.experimental import pallas as pl
from jax.experimental.pallas import tpu as pltpu
from jax.sharding import PartitionSpec as P

SHIFT = 5.0
ITERS = 3
DEPTH = ITERS + 1
LANES = 128


def ring(count, step):
    return [(i, (i + step) % count) for i in range(count)]


def pack_kernel(
    basis_hbm, guess_hbm, rhs_hbm, mask_hbm, east_hbm, north_hbm, surf_hbm,
    basis, sides, mask, to_n, to_s, to_e, to_w, sems,
):
    vectors, rows, cols = basis.shape
    moves = [(basis_hbm, basis), (mask_hbm, mask)]
    sources = (guess_hbm, rhs_hbm, east_hbm, north_hbm, surf_hbm)
    moves += [(source, sides.at[i]) for i, source in enumerate(sources)]
    copies = [pltpu.make_async_copy(a, b, sems.at[i]) for i, (a, b) in enumerate(moves)]
    for copy in copies:
        copy.start()
    for copy in copies:
        copy.wait()
    fields = [basis.at[k] for k in range(vectors)]
    fields += [sides.at[0], sides.at[1], mask, sides.at[2], sides.at[3], sides.at[4]]
    strip_e = jnp.zeros((rows, LANES), jnp.float32)
    strip_w = jnp.zeros((rows, LANES), jnp.float32)
    lane = lax.broadcasted_iota(jnp.int32, (rows, LANES), 1)
    for f, ref in enumerate(fields):
        at = DEPTH * f
        to_n[pl.ds(at, DEPTH), :] = ref[rows - DEPTH :, :].astype(jnp.float32)
        to_s[pl.ds(at, DEPTH), :] = ref[:DEPTH, :].astype(jnp.float32)
        here = (lane >= at) & (lane < at + DEPTH)
        last = ref[:, cols - LANES :].astype(jnp.float32)
        first = ref[:, :LANES].astype(jnp.float32)
        strip_e = jnp.where(here, pltpu.roll(last, (at + DEPTH) % LANES, 1), strip_e)
        strip_w = jnp.where(here, pltpu.roll(first, at, 1), strip_w)
    to_e[...] = strip_e
    to_w[...] = strip_w


def roll_lanes(v, by):
    return pltpu.roll(v, by % v.shape[1], 1)


def roll_rows(v, by):
    return pltpu.roll(v, by % v.shape[0], 0)


def apply_faces(v, diag, k_east, k_north):
    flux_e = k_east * (v - roll_lanes(v, -1))
    flux_n = k_north * (v - roll_rows(v, -1))
    return diag * v + (flux_e - roll_lanes(flux_e, 1)) + (flux_n - roll_rows(flux_n, 1))


def moments_kernel(
    place, basis, sides, mask,
    from_n, from_s, from_e, from_w, corner_n, corner_s,
    copies, basis_ext, side_ext, powers, fields_ext, faces, start_powers,
):
    vectors, rows, cols = basis.shape
    wide = cols + LANES
    tall = rows + 2 * DEPTH
    tiles = cols // LANES
    lane = lax.broadcasted_iota(jnp.int32, (tall, LANES), 1)
    strip_e = [from_e[...], corner_n[:DEPTH, :], corner_s[rows - DEPTH : rows, :]]
    strip_w = [from_w[...], corner_n[rows : rows + DEPTH, :], corner_s[2 * rows - DEPTH :, :]]
    strip_e = jnp.concatenate(strip_e, axis=0)
    strip_w = jnp.concatenate(strip_w, axis=0)

    def edge_of(f):
        at = DEPTH * f
        edge_e = pltpu.roll(strip_e, (-at) % LANES, 1)
        edge_w = pltpu.roll(strip_w, (LANES - DEPTH - at) % LANES, 1)
        return jnp.where(lane < DEPTH, edge_e, jnp.where(lane >= LANES - DEPTH, edge_w, 0.0))

    for k in range(vectors):
        at, to = DEPTH * k, tall * k
        for tile in range(tiles):
            part = pl.ds(tile * LANES, LANES)
            basis_ext[tile, pl.ds(to, rows), :] = basis[k, :, part]
            basis_ext[tile, pl.ds(to + rows, DEPTH), :] = from_n[pl.ds(at, DEPTH), part]
            basis_ext[tile, pl.ds(to + rows + DEPTH, DEPTH), :] = from_s[pl.ds(at, DEPTH), part]
        basis_ext[tiles, pl.ds(to, tall), :] = edge_of(k)
    own = (sides.at[0], sides.at[1], mask, sides.at[2], sides.at[3], sides.at[4])
    for f, ref in enumerate(own):
        at = DEPTH * (vectors + f)
        fields_ext[f, :rows, :cols] = ref[...].astype(jnp.float32)
        fields_ext[f, rows : rows + DEPTH, :cols] = from_n[pl.ds(at, DEPTH), :]
        fields_ext[f, rows + DEPTH :, :cols] = from_s[pl.ds(at, DEPTH), :]
        fields_ext[f, :, cols:] = edge_of(vectors + f)
    row = lax.broadcasted_iota(jnp.int32, (tall, wide), 0)
    beyond_n = (row >= rows) & (row < rows + DEPTH) & (place[0] == place[1] - 1)
    beyond_s = (row >= rows + DEPTH) & (place[0] == 0)
    wet = jnp.where(beyond_n | beyond_s, 0.0, fields_ext[2])
    k_east = fields_ext[3] * wet * roll_lanes(wet, -1)
    k_north = fields_ext[4] * wet * roll_rows(wet, -1)
    diag = fields_ext[5] * wet + (1.0 - wet)
    side_ext[0] = diag
    side_ext[1] = k_east
    side_ext[2] = k_north
    start = fields_ext[1] - apply_faces(fields_ext[0], diag, k_east, k_north)
    side_ext[3] = start
    v = start
    for power in range(ITERS + 1):
        for tile in range(tiles):
            part = v[:rows, tile * LANES : (tile + 1) * LANES]
            start_powers[tile, pl.ds(power * rows, rows), :] = part
        if power < ITERS:
            v = apply_faces(v, side_ext[0] - SHIFT, side_ext[1], side_ext[2])
    spare = (8 - (ITERS + 1)) * rows
    start_powers[:, pl.ds((ITERS + 1) * rows, spare), :] = jnp.zeros(
        (tiles, spare, LANES), jnp.float32
    )

    for q in range(tall):
        ring_row = (q - DEPTH) % tall
        for c, coeff in enumerate((side_ext.at[0], side_ext.at[1], side_ext.at[2])):
            spread = jnp.broadcast_to(coeff[ring_row : ring_row + 1, :], (8, wide))
            faces[c, q] = spread
            if c == 0:
                faces[3, q] = spread - SHIFT
        for tile in range(tiles + 1):
            part = basis_ext[tile, pl.ds(ring_row, vectors, stride=tall), :]
            powers[q, :vectors, tile * LANES : (tile + 1) * LANES] = part

    def coefficient(c, q):
        return jnp.concatenate([faces[c, q]] * (vectors // 8), axis=0)

    unroll = 2
    for power in range(DEPTH):
        first, last = 1 + power, tall - 1 - power
        source = slice(power * vectors, (power + 1) * vectors)
        target = slice((power + 1) * vectors, (power + 2) * vectors)
        middle = 0 if power == 0 else 3

        def some_rows(i, flux_s, first=first, source=source, target=target, middle=middle):
            for u in range(unroll):
                q = first + i * unroll + u
                v = powers[q, source, :]
                flux_n = coefficient(2, q) * (v - powers[q + 1, source, :])
                flux_e = coefficient(1, q) * (v - roll_lanes(v, -1))
                image = coefficient(middle, q) * v + (flux_e - roll_lanes(flux_e, 1))
                powers[q, target, :] = image + (flux_n - flux_s)
                flux_s = flux_n
            return flux_s

        below = first - 1
        flux = powers[below, source, :] - powers[first, source, :]
        lax.fori_loop(0, (last - first) // unroll, some_rows, coefficient(2, below) * flux)

    base = (ITERS + 2) * vectors
    count = base + 8
    batch = 4
    nt = (((1,), (1,)), ((), ()))

    def one_batch(i, carry):
        high_sum, cross_sum = carry
        x = []
        for u in range(batch):
            r = i * batch + u
            tail = [start_powers[t, pl.ds(r, 8, stride=rows), :] for t in range(tiles)]
            tail = jnp.concatenate(tail, axis=1)
            x.append(jnp.concatenate([powers[r + DEPTH, :, :cols], tail], axis=0))
        x = jnp.concatenate(x, axis=1)
        high = x.astype(jnp.bfloat16)
        low = (x - high.astype(jnp.float32)).astype(jnp.bfloat16)
        high_sum += lax.dot_general(high, high, nt, preferred_element_type=jnp.float32)
        cross_sum += lax.dot_general(high, low, nt, preferred_element_type=jnp.float32)
        return high_sum, cross_sum

    zero = jnp.zeros((count, count), jnp.float32)
    high_sum, cross_sum = lax.fori_loop(0, rows // batch, one_batch, (zero, zero))
    full = high_sum + cross_sum + cross_sum.T
    full = jnp.concatenate([full, jnp.zeros((count, LANES - count), jnp.float32)], axis=1)
    at = lax.broadcasted_iota(jnp.int32, (vectors, LANES), 1)
    slabs = [full[a * vectors : (a + 1) * vectors, :] for a in range(4)]
    tail = jnp.concatenate([full[base:, :], jnp.zeros((vectors - 8, LANES), jnp.float32)], axis=0)
    out = jnp.zeros((vectors, LANES), jnp.float32)

    def move(out, v, first, width, target):
        moved = pltpu.roll(v, (target - first) % LANES, 1)
        return jnp.where((at >= target) & (at < target + width), moved, out)

    out = move(out, slabs[0], vectors, vectors, 0)
    out = move(out, slabs[1], vectors, 2 * vectors, vectors)
    out = move(out, slabs[2], 2 * vectors, 2 * vectors, 3 * vectors)
    out = move(out, slabs[3], 3 * vectors, 2 * vectors, 5 * vectors)
    free = 7 * vectors
    out = move(out, slabs[0], base, 1, free)
    out = move(out, slabs[1], base, 2, free + 1)
    out = move(out, slabs[2], base + 1, 2, free + 3)
    out = move(out, slabs[3], base + 2, 2, free + 5)
    out = move(out, tail, base, 4, free + 8)

    def one_copy(device, carry):
        copies[device] = out
        return carry

    lax.fori_loop(0, copies.shape[0], one_copy, 0, unroll=8)


def finish_kernel(parts, sides, basis_ext, side_ext, solution, residual, spread):
    _, tall, wide = side_ext.shape
    _, rows, cols = sides.shape
    vectors = basis_ext.shape[1] // tall
    free = 7 * vectors
    several = 8

    def add_parts(i, sums):
        return tuple(sums[n] + parts[i * several + n] for n in range(several))

    nothing = (jnp.zeros(parts.shape[1:], jnp.float32),) * several
    sums = list(lax.fori_loop(0, parts.shape[0] // several, add_parts, nothing, unroll=2))
    while len(sums) > 1:
        sums = [sums[i] + sums[i + 1] for i in range(0, len(sums), 2)]
    total = sums[0]
    lane = lax.broadcasted_iota(jnp.int32, (vectors, LANES), 1)
    sub = lax.broadcasted_iota(jnp.int32, (vectors, LANES), 0)
    table = total
    for i in range(vectors):
        column = table[:, i : i + 1]
        pivot_row = table[i : i + 1, :] / table[i : i + 1, i : i + 1]
        table = jnp.where(sub == i, pivot_row, table - column * pivot_row)
    own_lane = (lane % vectors) == sub
    z = [-table[:, free : free + 1]]
    sums = jnp.zeros((vectors, LANES), jnp.float32)
    history = jnp.zeros((1, LANES), jnp.float32)
    lane_row = lane[:1, :]
    for j in range(2 * ITERS):
        newest = jnp.sum(jnp.where(own_lane, z[j], 0.0), axis=0, keepdims=True)
        history = pltpu.roll(history, vectors, 1)
        history = jnp.where((lane_row >= vectors) & (lane_row < 2 * vectors), newest, history)
        terms = (lane >= vectors) & (lane < (j + 2) * vectors)
        weights = jnp.where(terms, history, jnp.where(lane == free + 1 + j, 1.0, 0.0))
        z.append(-jnp.sum(table * weights, axis=1, keepdims=True))
    for j in range(2 * ITERS + 1):
        sums = sums + pltpu.roll(jnp.where(lane >= free, total, 0.0) * z[j], j, 1)
    picked = jnp.where((lane > free) & (lane < free + 7), sums, 0.0)
    for a in range(ITERS):
        moved = pltpu.roll(total, (a - 7) % LANES, 1)
        first = free + 1 + 2 * a
        picked += jnp.where((sub == a) & (lane >= first) & (lane < first + 2), moved, 0.0)
    moment_row = jnp.sum(picked, axis=0, keepdims=True)
    mu = [moment_row[:, free + 1 + k : free + 2 + k] for k in range(2 * ITERS)]
    for i in range(ITERS + 1):
        spread[i] = jnp.broadcast_to(z[i], (vectors, LANES))

    nil = jnp.zeros((1, 1), jnp.float32)
    rho = [nil + 1.0] + [nil] * ITERS
    gamma = [nil] * (ITERS + 1)
    delta = [nil] * ITERS
    curv = nil
    prev = nil
    for j in range(ITERS):
        norm = nil
        image = nil
        for a in range(j + 1):
            for b in range(j + 1):
                pair = rho[a] * rho[b]
                norm += pair * mu[a + b]
                image += pair * (mu[a + b + 1] + SHIFT * mu[a + b])
        if j == 0:
            gamma = list(rho)
            curv = image
        else:
            ratio = norm / prev
            gamma = [rho[i] + ratio * gamma[i] for i in range(ITERS + 1)]
            curv = image - ratio * ratio * curv
        step = norm / curv
        delta = [delta[i] + step * gamma[i] for i in range(ITERS)]
        below = [nil] + gamma[:ITERS]
        rho = [rho[i] - step * (SHIFT * gamma[i] + below[i]) for i in range(ITERS + 1)]
        prev = norm

    along = [[] for _ in range(ITERS + 1)]
    for tile in range(wide // LANES):
        acc = [jnp.zeros((tall, LANES), jnp.float32) for _ in range(ITERS + 1)]
        for k in range(vectors):
            w = basis_ext[tile, pl.ds(tall * k, tall), :]
            for i in range(ITERS + 1):
                acc[i] = acc[i] + w * spread[i, pl.ds(k, 1), :]
        for i in range(ITERS + 1):
            along[i].append(acc[i])
    along = [jnp.concatenate(pieces, axis=1) for pieces in along]
    diag, k_east, k_north = side_ext[0], side_ext[1], side_ext[2]
    image = functools.partial(apply_faces, k_east=k_east, k_north=k_north)
    v = side_ext[3] + image(along[0], diag)
    x = sides[0] - along[0][:rows, :cols]
    r = rho[0] * v[:rows, :cols]
    for i in range(ITERS):
        x = x + delta[i] * (v + along[i + 1])[:rows, :cols]
        v = image(v, diag - SHIFT) + image(along[i + 1], diag)
        r = r + rho[i + 1] * v[:rows, :cols]
    solution[...] = x
    residual[...] = r


def call(kernel, out_shape, spaces, inputs, scratch=(), name=None):
    return pl.pallas_call(
        kernel,
        out_shape=out_shape,
        in_specs=[pl.BlockSpec(memory_space=space) for space in spaces],
        out_specs=[pl.BlockSpec(memory_space=pltpu.VMEM)] * len(out_shape),
        scratch_shapes=scratch,
        name=name,
        compiler_params=pltpu.CompilerParams(vmem_limit_bytes=24 * 1024 * 1024),
    )(*inputs)


def f32(*shape):
    return jax.ShapeDtypeStruct(shape, jnp.float32)


def shards(right_side, first_guess, cell_mask, cond_east, cond_north, surface, recycled):
    vectors, rows, cols = recycled.shape
    n_lat, n_lon = lax.axis_size("lat"), lax.axis_size("lon")
    devices = n_lat * n_lon
    fields = vectors + 6
    tall, wide = rows + 2 * DEPTH, cols + LANES
    tiles = cols // LANES
    own = (recycled, first_guess, right_side, cell_mask, cond_east, cond_north, surface)
    band, strip = f32(fields * DEPTH, cols), f32(rows, LANES)
    basis, sides, mask, to_n, to_s, to_e, to_w = call(
        pack_kernel,
        [f32(vectors, rows, cols), f32(5, rows, cols), jax.ShapeDtypeStruct((rows, cols), jnp.int32)]
        + [band, band, strip, strip],
        [pltpu.HBM] * 7,
        [pltpu.with_memory_space_constraint(array, pltpu.HBM) for array in own],
        scratch=[pltpu.SemaphoreType.DMA((7,))],
        name="pack",
    )
    north, south = ring(n_lat, 1), ring(n_lat, -1)
    from_w = lax.ppermute(to_e, "lon", ring(n_lon, 1))
    from_e = lax.ppermute(to_w, "lon", ring(n_lon, -1))
    from_s = lax.ppermute(to_n, "lat", north)
    from_n = lax.ppermute(to_s, "lat", south)
    strips = jnp.concatenate([from_e, from_w], axis=0)
    corner_s = lax.ppermute(strips, "lat", north)
    corner_n = lax.ppermute(strips, "lat", south)
    place = jnp.stack([lax.axis_index("lat"), jnp.int32(n_lat)])
    copies, basis_ext, side_ext = call(
        moments_kernel,
        [f32(devices, vectors, LANES), f32(tiles + 1, vectors * tall, LANES), f32(4, tall, wide)],
        [pltpu.SMEM] + [pltpu.VMEM] * 9,
        (place, basis, sides, mask, from_n, from_s, from_e, from_w, corner_n, corner_s),
        scratch=[
            pltpu.VMEM((tall, (ITERS + 2) * vectors, wide), jnp.float32),
            pltpu.VMEM((6, tall, wide), jnp.float32),
            pltpu.VMEM((4, tall, 8, wide), jnp.float32),
            pltpu.VMEM((tiles, 8 * rows, LANES), jnp.float32),
        ],
        name="moments",
    )
    parts = lax.all_to_all(copies, ("lat", "lon"), 0, 0)
    return call(
        finish_kernel,
        [f32(rows, cols), f32(rows, cols)],
        [pltpu.VMEM] * 4,
        (parts, sides, basis_ext, side_ext),
        scratch=[pltpu.VMEM((ITERS + 1, vectors, LANES), jnp.float32)],
        name="finish",
    )


def solution(mesh):
    block = P("lat", "lon")
    return jax.shard_map(
        shards,
        mesh=mesh,
        in_specs=(block,) * 6 + (P(None, "lat", "lon"),),
        out_specs=(block, block),
        check_vma=False,
    )
```

```python
import jax
import jax.numpy as jnp
from jax import lax
from jax.experimental import pallas as pl
from jax.experimental.pallas import tpu as pltpu
from jax.sharding import PartitionSpec as P

SHIFT = 5.0
ITERS = 3
DEPTH = ITERS + 1
LANES = 128
UNROLL = (11, 10, 9, 8)


def ring(count, step):
    return [(i, (i + step) % count) for i in range(count)]


def pack_kernel(
    basis_hbm, guess_hbm, rhs_hbm, mask_hbm, east_hbm, north_hbm, surf_hbm,
    basis, sides, mask, to_n, to_s, to_e, to_w, sems,
):
    vectors, rows, cols = basis.shape
    moves = [(basis_hbm, basis), (mask_hbm, mask)]
    sources = (guess_hbm, rhs_hbm, east_hbm, north_hbm, surf_hbm)
    moves += [(source, sides.at[i]) for i, source in enumerate(sources)]
    copies = [pltpu.make_async_copy(a, b, sems.at[i]) for i, (a, b) in enumerate(moves)]
    for copy in copies:
        copy.start()
    for copy in copies:
        copy.wait()
    fields = [basis.at[k] for k in range(vectors)]
    fields += [sides.at[0], sides.at[1], mask, sides.at[2], sides.at[3], sides.at[4]]
    strip_e = jnp.zeros((rows, LANES), jnp.float32)
    strip_w = jnp.zeros((rows, LANES), jnp.float32)
    lane = lax.broadcasted_iota(jnp.int32, (rows, LANES), 1)
    for f, ref in enumerate(fields):
        at = DEPTH * f
        to_n[pl.ds(at, DEPTH), :] = ref[rows - DEPTH :, :].astype(jnp.float32)
        to_s[pl.ds(at, DEPTH), :] = ref[:DEPTH, :].astype(jnp.float32)
        here = (lane >= at) & (lane < at + DEPTH)
        last = ref[:, cols - LANES :].astype(jnp.float32)
        first = ref[:, :LANES].astype(jnp.float32)
        strip_e = jnp.where(here, pltpu.roll(last, (at + DEPTH) % LANES, 1), strip_e)
        strip_w = jnp.where(here, pltpu.roll(first, at, 1), strip_w)
    to_e[...] = strip_e
    to_w[...] = strip_w


def roll_lanes(v, by):
    return pltpu.roll(v, by % v.shape[1], 1)


def roll_rows(v, by):
    return pltpu.roll(v, by % v.shape[0], 0)


def apply_faces(v, faces, shift=0.0):
    centre, k_east, k_west, k_north, k_south = faces
    beside = k_east * roll_lanes(v, -1) + k_west * roll_lanes(v, 1)
    above = k_north * roll_rows(v, -1) + k_south * roll_rows(v, 1)
    return (centre - shift) * v - (beside + above)


def moments_kernel(
    place, basis, sides, mask,
    from_n, from_s, from_e, from_w, corner_n, corner_s,
    copies, basis_ext, side_ext, powers, fields_ext, faces, start_powers,
):
    vectors, rows, cols = basis.shape
    wide = cols + LANES
    tall = rows + 2 * DEPTH
    tiles = cols // LANES
    lane = lax.broadcasted_iota(jnp.int32, (tall, LANES), 1)
    strip_e = [from_e[...], corner_n[:DEPTH, :], corner_s[rows - DEPTH : rows, :]]
    strip_w = [from_w[...], corner_n[rows : rows + DEPTH, :], corner_s[2 * rows - DEPTH :, :]]
    strip_e = jnp.concatenate(strip_e, axis=0)
    strip_w = jnp.concatenate(strip_w, axis=0)

    def edge_of(f):
        at = DEPTH * f
        edge_e = pltpu.roll(strip_e, (-at) % LANES, 1)
        edge_w = pltpu.roll(strip_w, (LANES - DEPTH - at) % LANES, 1)
        return jnp.where(lane < DEPTH, edge_e, jnp.where(lane >= LANES - DEPTH, edge_w, 0.0))

    for k in range(vectors):
        at, to = DEPTH * k, tall * k
        for tile in range(tiles):
            part = pl.ds(tile * LANES, LANES)
            basis_ext[tile, pl.ds(to, rows), :] = basis[k, :, part]
            basis_ext[tile, pl.ds(to + rows, DEPTH), :] = from_n[pl.ds(at, DEPTH), part]
            basis_ext[tile, pl.ds(to + rows + DEPTH, DEPTH), :] = from_s[pl.ds(at, DEPTH), part]
        basis_ext[tiles, pl.ds(to, tall), :] = edge_of(k)
    own = (sides.at[0], sides.at[1], mask, sides.at[2], sides.at[3], sides.at[4])
    for f, ref in enumerate(own):
        at = DEPTH * (vectors + f)
        fields_ext[f, :rows, :cols] = ref[...].astype(jnp.float32)
        fields_ext[f, rows : rows + DEPTH, :cols] = from_n[pl.ds(at, DEPTH), :]
        fields_ext[f, rows + DEPTH :, :cols] = from_s[pl.ds(at, DEPTH), :]
        fields_ext[f, :, cols:] = edge_of(vectors + f)
    row = lax.broadcasted_iota(jnp.int32, (tall, wide), 0)
    beyond_n = (row >= rows) & (row < rows + DEPTH) & (place[0] == place[1] - 1)
    beyond_s = (row >= rows + DEPTH) & (place[0] == 0)
    wet = jnp.where(beyond_n | beyond_s, 0.0, fields_ext[2])
    k_east = fields_ext[3] * wet * roll_lanes(wet, -1)
    k_north = fields_ext[4] * wet * roll_rows(wet, -1)
    k_west = roll_lanes(k_east, 1)
    k_south = roll_rows(k_north, 1)
    centre = fields_ext[5] * wet + k_east + k_west + k_north + k_south + (1.0 - wet)
    for c, values in enumerate((centre, k_east, k_west, k_north, k_south)):
        side_ext[c] = values
    start = fields_ext[1] - apply_faces(fields_ext[0], [side_ext[c] for c in range(5)])
    side_ext[5] = start
    v = start
    for power in range(ITERS + 1):
        for tile in range(tiles):
            part = v[:rows, tile * LANES : (tile + 1) * LANES]
            start_powers[tile, pl.ds(power * rows, rows), :] = part
        if power < ITERS:
            v = apply_faces(v, [side_ext[c] for c in range(5)], SHIFT)
    spare = (8 - (ITERS + 1)) * rows
    start_powers[:, pl.ds((ITERS + 1) * rows, spare), :] = jnp.zeros(
        (tiles, spare, LANES), jnp.float32
    )

    for q in range(tall):
        ring_row = (q - DEPTH) % tall
        for c in range(4):
            spread = jnp.broadcast_to(side_ext[c, ring_row : ring_row + 1, :], (8, wide))
            faces[c, q] = spread
            if c == 0:
                faces[4, q] = spread - SHIFT
        for tile in range(tiles + 1):
            part = basis_ext[tile, pl.ds(ring_row, vectors, stride=tall), :]
            powers[q, :vectors, tile * LANES : (tile + 1) * LANES] = part

    def coefficient(c, q):
        return jnp.concatenate([faces[c, q]] * (vectors // 8), axis=0)

    for power in range(DEPTH):
        first, last = 1 + power, tall - 1 - power
        source = slice(power * vectors, (power + 1) * vectors)
        target = slice((power + 1) * vectors, (power + 2) * vectors)
        middle = 0 if power == 0 else 4
        unroll = UNROLL[power]

        def some_rows(i, carry, source=source, target=target, middle=middle, first=first, unroll=unroll):
            for u in range(unroll):
                q = first + i * unroll + u
                v = powers[q, source, :]
                beside = coefficient(1, q) * roll_lanes(v, -1) + coefficient(2, q) * roll_lanes(v, 1)
                above = coefficient(3, q) * powers[q + 1, source, :]
                above += coefficient(3, q - 1) * powers[q - 1, source, :]
                powers[q, target, :] = coefficient(middle, q) * v - (beside + above)
            return carry

        lax.fori_loop(0, (last - first) // unroll, some_rows, 0)

    base = (ITERS + 2) * vectors
    count = base + 8
    batch = 4
    nt = (((1,), (1,)), ((), ()))

    def one_batch(i, carry):
        high_sum, cross_sum = carry
        x = []
        for u in range(batch):
            r = i * batch + u
            tail = [start_powers[t, pl.ds(r, 8, stride=rows), :] for t in range(tiles)]
            tail = jnp.concatenate(tail, axis=1)
            x.append(jnp.concatenate([powers[r + DEPTH, :, :cols], tail], axis=0))
        x = jnp.concatenate(x, axis=1)
        high = x.astype(jnp.bfloat16)
        low = (x - high.astype(jnp.float32)).astype(jnp.bfloat16)
        high_sum += lax.dot_general(high, high, nt, preferred_element_type=jnp.float32)
        cross_sum += lax.dot_general(high, low, nt, preferred_element_type=jnp.float32)
        return high_sum, cross_sum

    zero = jnp.zeros((count, count), jnp.float32)
    high_sum, cross_sum = lax.fori_loop(0, rows // batch, one_batch, (zero, zero))
    full = high_sum + cross_sum + cross_sum.T
    full = jnp.concatenate([full, jnp.zeros((count, LANES - count), jnp.float32)], axis=1)
    at = lax.broadcasted_iota(jnp.int32, (vectors, LANES), 1)
    slabs = [full[a * vectors : (a + 1) * vectors, :] for a in range(4)]
    tail = jnp.concatenate([full[base:, :], jnp.zeros((vectors - 8, LANES), jnp.float32)], axis=0)
    out = jnp.zeros((vectors, LANES), jnp.float32)

    def move(out, v, first, width, target):
        moved = pltpu.roll(v, (target - first) % LANES, 1)
        return jnp.where((at >= target) & (at < target + width), moved, out)

    out = move(out, slabs[0], vectors, vectors, 0)
    out = move(out, slabs[1], vectors, 2 * vectors, vectors)
    out = move(out, slabs[2], 2 * vectors, 2 * vectors, 3 * vectors)
    out = move(out, slabs[3], 3 * vectors, 2 * vectors, 5 * vectors)
    free = 7 * vectors
    out = move(out, slabs[0], base, 1, free)
    out = move(out, slabs[1], base, 2, free + 1)
    out = move(out, slabs[2], base + 1, 2, free + 3)
    out = move(out, slabs[3], base + 2, 2, free + 5)
    out = move(out, tail, base, 4, free + 8)

    def one_copy(device, carry):
        copies[device] = out
        return carry

    lax.fori_loop(0, copies.shape[0], one_copy, 0, unroll=8)


def finish_kernel(parts, sides, basis_ext, side_ext, solution, residual, spread):
    _, tall, wide = side_ext.shape
    _, rows, cols = sides.shape
    vectors = basis_ext.shape[1] // tall
    free = 7 * vectors
    several = 8

    def add_parts(i, sums):
        return tuple(sums[n] + parts[i * several + n] for n in range(several))

    nothing = (jnp.zeros(parts.shape[1:], jnp.float32),) * several
    sums = list(lax.fori_loop(0, parts.shape[0] // several, add_parts, nothing, unroll=2))
    while len(sums) > 1:
        sums = [sums[i] + sums[i + 1] for i in range(0, len(sums), 2)]
    total = sums[0]
    lane = lax.broadcasted_iota(jnp.int32, (vectors, LANES), 1)
    sub = lax.broadcasted_iota(jnp.int32, (vectors, LANES), 0)
    table = total
    for i in range(vectors):
        column = table[:, i : i + 1]
        pivot_row = table[i : i + 1, :] / table[i : i + 1, i : i + 1]
        table = jnp.where(sub == i, pivot_row, table - column * pivot_row)
    own_lane = (lane % vectors) == sub
    z = [-table[:, free : free + 1]]
    sums = jnp.zeros((vectors, LANES), jnp.float32)
    history = jnp.zeros((1, LANES), jnp.float32)
    lane_row = lane[:1, :]
    for j in range(2 * ITERS):
        newest = jnp.sum(jnp.where(own_lane, z[j], 0.0), axis=0, keepdims=True)
        history = pltpu.roll(history, vectors, 1)
        history = jnp.where((lane_row >= vectors) & (lane_row < 2 * vectors), newest, history)
        terms = (lane >= vectors) & (lane < (j + 2) * vectors)
        weights = jnp.where(terms, history, jnp.where(lane == free + 1 + j, 1.0, 0.0))
        z.append(-jnp.sum(table * weights, axis=1, keepdims=True))
    for j in range(2 * ITERS + 1):
        sums = sums + pltpu.roll(jnp.where(lane >= free, total, 0.0) * z[j], j, 1)
    picked = jnp.where((lane > free) & (lane < free + 7), sums, 0.0)
    for a in range(ITERS):
        moved = pltpu.roll(total, (a - 7) % LANES, 1)
        first = free + 1 + 2 * a
        picked += jnp.where((sub == a) & (lane >= first) & (lane < first + 2), moved, 0.0)
    moment_row = jnp.sum(picked, axis=0, keepdims=True)
    mu = [moment_row[:, free + 1 + k : free + 2 + k] for k in range(2 * ITERS)]
    for i in range(ITERS + 1):
        spread[i] = jnp.broadcast_to(z[i], (vectors, LANES))

    nil = jnp.zeros((1, 1), jnp.float32)
    rho = [nil + 1.0] + [nil] * ITERS
    gamma = [nil] * (ITERS + 1)
    delta = [nil] * ITERS
    curv = nil
    prev = nil
    for j in range(ITERS):
        norm = nil
        image = nil
        for a in range(j + 1):
            for b in range(j + 1):
                pair = rho[a] * rho[b]
                norm += pair * mu[a + b]
                image += pair * (mu[a + b + 1] + SHIFT * mu[a + b])
        if j == 0:
            gamma = list(rho)
            curv = image
        else:
            ratio = norm / prev
            gamma = [rho[i] + ratio * gamma[i] for i in range(ITERS + 1)]
            curv = image - ratio * ratio * curv
        step = norm / curv
        delta = [delta[i] + step * gamma[i] for i in range(ITERS)]
        below = [nil] + gamma[:ITERS]
        rho = [rho[i] - step * (SHIFT * gamma[i] + below[i]) for i in range(ITERS + 1)]
        prev = norm

    along = [[] for _ in range(ITERS + 1)]
    for tile in range(wide // LANES):
        acc = [jnp.zeros((tall, LANES), jnp.float32) for _ in range(ITERS + 1)]
        for k in range(vectors):
            w = basis_ext[tile, pl.ds(tall * k, tall), :]
            for i in range(ITERS + 1):
                acc[i] = acc[i] + w * spread[i, pl.ds(k, 1), :]
        for i in range(ITERS + 1):
            along[i].append(acc[i])
    along = [jnp.concatenate(pieces, axis=1) for pieces in along]
    faces = [side_ext[c] for c in range(5)]
    v = side_ext[5] + apply_faces(along[0], faces)
    x = sides[0] - along[0][:rows, :cols]
    r = rho[0] * v[:rows, :cols]
    for i in range(ITERS):
        x = x + delta[i] * (v + along[i + 1])[:rows, :cols]
        v = apply_faces(v, faces, SHIFT) + apply_faces(along[i + 1], faces)
        r = r + rho[i + 1] * v[:rows, :cols]
    solution[...] = x
    residual[...] = r


def call(kernel, out_shape, spaces, inputs, scratch=(), name=None):
    return pl.pallas_call(
        kernel,
        out_shape=out_shape,
        in_specs=[pl.BlockSpec(memory_space=space) for space in spaces],
        out_specs=[pl.BlockSpec(memory_space=pltpu.VMEM)] * len(out_shape),
        scratch_shapes=scratch,
        name=name,
        compiler_params=pltpu.CompilerParams(vmem_limit_bytes=24 * 1024 * 1024),
    )(*inputs)


def f32(*shape):
    return jax.ShapeDtypeStruct(shape, jnp.float32)


def shards(right_side, first_guess, cell_mask, cond_east, cond_north, surface, recycled):
    vectors, rows, cols = recycled.shape
    n_lat, n_lon = lax.axis_size("lat"), lax.axis_size("lon")
    devices = n_lat * n_lon
    fields = vectors + 6
    tall, wide = rows + 2 * DEPTH, cols + LANES
    tiles = cols // LANES
    own = (recycled, first_guess, right_side, cell_mask, cond_east, cond_north, surface)
    band, strip = f32(fields * DEPTH, cols), f32(rows, LANES)
    basis, sides, mask, to_n, to_s, to_e, to_w = call(
        pack_kernel,
        [f32(vectors, rows, cols), f32(5, rows, cols), jax.ShapeDtypeStruct((rows, cols), jnp.int32)]
        + [band, band, strip, strip],
        [pltpu.HBM] * 7,
        [pltpu.with_memory_space_constraint(array, pltpu.HBM) for array in own],
        scratch=[pltpu.SemaphoreType.DMA((7,))],
        name="pack",
    )
    north, south = ring(n_lat, 1), ring(n_lat, -1)
    from_w = lax.ppermute(to_e, "lon", ring(n_lon, 1))
    from_e = lax.ppermute(to_w, "lon", ring(n_lon, -1))
    from_s = lax.ppermute(to_n, "lat", north)
    from_n = lax.ppermute(to_s, "lat", south)
    strips = jnp.concatenate([from_e, from_w], axis=0)
    corner_s = lax.ppermute(strips, "lat", north)
    corner_n = lax.ppermute(strips, "lat", south)
    place = jnp.stack([lax.axis_index("lat"), jnp.int32(n_lat)])
    copies, basis_ext, side_ext = call(
        moments_kernel,
        [f32(devices, vectors, LANES), f32(tiles + 1, vectors * tall, LANES), f32(6, tall, wide)],
        [pltpu.SMEM] + [pltpu.VMEM] * 9,
        (place, basis, sides, mask, from_n, from_s, from_e, from_w, corner_n, corner_s),
        scratch=[
            pltpu.VMEM((tall, (ITERS + 2) * vectors, wide), jnp.float32),
            pltpu.VMEM((6, tall, wide), jnp.float32),
            pltpu.VMEM((5, tall, 8, wide), jnp.float32),
            pltpu.VMEM((tiles, 8 * rows, LANES), jnp.float32),
        ],
        name="moments",
    )
    parts = lax.all_to_all(copies, ("lat", "lon"), 0, 0)
    return call(
        finish_kernel,
        [f32(rows, cols), f32(rows, cols)],
        [pltpu.VMEM] * 4,
        (parts, sides, basis_ext, side_ext),
        scratch=[pltpu.VMEM((ITERS + 1, vectors, LANES), jnp.float32)],
        name="finish",
    )


def solution(mesh):
    block = P("lat", "lon")
    return jax.shard_map(
        shards,
        mesh=mesh,
        in_specs=(block,) * 6 + (P(None, "lat", "lon"),),
        out_specs=(block, block),
        check_vma=False,
    )
```

```python
import jax
import jax.numpy as jnp
from jax import lax
from jax.experimental import pallas as pl
from jax.experimental.pallas import tpu as pltpu
from jax.sharding import PartitionSpec as P

SHIFT = 5.0
ITERS = 3
DEPTH = ITERS + 1
LANES = 128


def ring(count, step):
    return [(i, (i + step) % count) for i in range(count)]


def pack_kernel(
    basis_hbm, guess_hbm, rhs_hbm, mask_hbm, east_hbm, north_hbm, surf_hbm,
    basis, sides, mask, to_n, to_s, to_e, to_w, sems,
):
    vectors, rows, cols = basis.shape
    moves = [(basis_hbm, basis), (mask_hbm, mask)]
    sources = (guess_hbm, rhs_hbm, east_hbm, north_hbm, surf_hbm)
    moves += [(source, sides.at[i]) for i, source in enumerate(sources)]
    copies = [pltpu.make_async_copy(a, b, sems.at[i]) for i, (a, b) in enumerate(moves)]
    for copy in copies:
        copy.start()
    for copy in copies:
        copy.wait()
    fields = [basis.at[k] for k in range(vectors)]
    fields += [sides.at[0], sides.at[1], mask, sides.at[2], sides.at[3], sides.at[4]]
    strip_e = jnp.zeros((rows, LANES), jnp.float32)
    strip_w = jnp.zeros((rows, LANES), jnp.float32)
    lane = lax.broadcasted_iota(jnp.int32, (rows, LANES), 1)
    for f, ref in enumerate(fields):
        at = DEPTH * f
        to_n[pl.ds(at, DEPTH), :] = ref[rows - DEPTH :, :].astype(jnp.float32)
        to_s[pl.ds(at, DEPTH), :] = ref[:DEPTH, :].astype(jnp.float32)
        here = (lane >= at) & (lane < at + DEPTH)
        last = ref[:, cols - LANES :].astype(jnp.float32)
        first = ref[:, :LANES].astype(jnp.float32)
        strip_e = jnp.where(here, pltpu.roll(last, (at + DEPTH) % LANES, 1), strip_e)
        strip_w = jnp.where(here, pltpu.roll(first, at, 1), strip_w)
    to_e[...] = strip_e
    to_w[...] = strip_w


def roll_lanes(v, by):
    return pltpu.roll(v, by % v.shape[1], 1)


def roll_rows(v, by):
    return pltpu.roll(v, by % v.shape[0], 0)


def apply_faces(v, faces, shift=0.0):
    centre, k_east, k_west, k_north, k_south = faces
    beside = k_east * roll_lanes(v, -1) + k_west * roll_lanes(v, 1)
    above = k_north * roll_rows(v, -1) + k_south * roll_rows(v, 1)
    return (centre - shift) * v - (beside + above)


def edges(f, strip_e, strip_w):
    at = DEPTH * f
    lane = lax.broadcasted_iota(jnp.int32, strip_e.shape, 1)
    edge_e = pltpu.roll(strip_e, (-at) % LANES, 1)
    edge_w = pltpu.roll(strip_w, (LANES - DEPTH - at) % LANES, 1)
    return jnp.where(lane < DEPTH, edge_e, jnp.where(lane >= LANES - DEPTH, edge_w, 0.0))


def faces_of(wet, east, north, surf):
    k_east = east * wet * roll_lanes(wet, -1)
    k_north = north * wet * roll_rows(wet, -1)
    k_west = roll_lanes(k_east, 1)
    k_south = roll_rows(k_north, 1)
    centre = surf * wet + k_east + k_west + k_north + k_south + (1.0 - wet)
    return centre, k_east, k_west, k_north, k_south


def spread_faces(side, faces, q, row):
    for c in range(4):
        line = side[c, row : row + 1, :]
        spread = jnp.broadcast_to(line, (8, line.shape[1]))
        faces[c, q] = spread
        if c == 0:
            faces[4, q] = spread - SHIFT


def power_rows(powers, faces, power, q, vectors):
    source = slice(power * vectors, (power + 1) * vectors)
    target = slice((power + 1) * vectors, (power + 2) * vectors)

    def coefficient(c, q):
        return jnp.concatenate([faces[c, q]] * (vectors // 8), axis=0)

    v = powers[q, source, :]
    beside = coefficient(1, q) * roll_lanes(v, -1) + coefficient(2, q) * roll_lanes(v, 1)
    above = coefficient(3, q) * powers[q + 1, source, :]
    above += coefficient(3, q - 1) * powers[q - 1, source, :]
    middle = coefficient(0 if power == 0 else 4, q)
    powers[q, target, :] = middle * v - (beside + above)


def keep_start_powers(v, faces, rows, start_powers):
    tiles = start_powers.shape[0]
    for power in range(ITERS + 1):
        for tile in range(tiles):
            part = v[:rows, tile * LANES : (tile + 1) * LANES]
            start_powers[tile, pl.ds(power * rows, rows), :] = part
        if power < ITERS:
            v = apply_faces(v, faces, SHIFT)
    spare = (8 - (ITERS + 1)) * rows
    start_powers[:, pl.ds((ITERS + 1) * rows, spare), :] = jnp.zeros(
        (tiles, spare, LANES), jnp.float32
    )


def products(powers, start_powers, batches, rows):
    tiles = start_powers.shape[0]
    nt = (((1,), (1,)), ((), ()))
    high_sum = 0.0
    cross_sum = 0.0
    for batch in batches:
        x = []
        for r in batch:
            tail = [start_powers[t, pl.ds(r, 8, stride=rows), :] for t in range(tiles)]
            tail = jnp.concatenate(tail, axis=1)
            x.append(jnp.concatenate([powers[r + DEPTH, :, : tiles * LANES], tail], axis=0))
        x = jnp.concatenate(x, axis=1)
        high = x.astype(jnp.bfloat16)
        low = (x - high.astype(jnp.float32)).astype(jnp.bfloat16)
        high_sum += lax.dot_general(high, high, nt, preferred_element_type=jnp.float32)
        cross_sum += lax.dot_general(high, low, nt, preferred_element_type=jnp.float32)
    return high_sum, cross_sum


def inner_kernel(
    basis, sides, mask, from_e, from_w,
    powers, basis_ext, sums, side, faces, start_powers,
):
    vectors, rows, cols = basis.shape
    tall = rows + 2 * DEPTH
    tiles = cols // LANES
    strip_e, strip_w = from_e[...], from_w[...]
    for k in range(vectors):
        for tile in range(tiles):
            basis_ext[tile, pl.ds(tall * k, rows), :] = basis[k, :, tile * LANES : (tile + 1) * LANES]
        basis_ext[tiles, pl.ds(tall * k, rows), :] = edges(k, strip_e, strip_w)
    own = (sides[0], sides[1], mask[...].astype(jnp.float32), sides[2], sides[3], sides[4])
    guess, rhs, wet, east, north, surf = [
        jnp.concatenate([v, edges(vectors + f, strip_e, strip_w)], axis=1)
        for f, v in enumerate(own)
    ]
    for c, values in enumerate(faces_of(wet, east, north, surf)):
        side[c] = values
    for row in range(rows):
        spread_faces(side, faces, row + DEPTH, row)
        for tile in range(tiles + 1):
            part = basis_ext[tile, pl.ds(row, vectors, stride=tall), :]
            powers[row + DEPTH, :vectors, tile * LANES : (tile + 1) * LANES] = part
    whole = [side[c] for c in range(5)]
    keep_start_powers(rhs - apply_faces(guess, whole), whole, rows, start_powers)
    for power in range(DEPTH):
        first, last = DEPTH + 1 + power, DEPTH + rows - 1 - power
        unroll = (last - first) // (2 if power < 2 else 1)

        def some_rows(i, carry, power=power, first=first, unroll=unroll):
            for u in range(unroll):
                power_rows(powers, faces, power, first + i * unroll + u, vectors)
            return carry

        lax.fori_loop(0, (last - first) // unroll, some_rows, 0)
    middle = range(DEPTH, rows - DEPTH)
    batches = [middle[at : at + DEPTH] for at in range(0, len(middle), DEPTH)]
    high_sum, cross_sum = products(powers, start_powers, batches, rows)
    sums[0] = high_sum
    sums[1] = cross_sum


def outer_kernel(
    place, basis_in, powers_in, sums, sides, mask,
    from_n, from_s, from_e, from_w, corner_n, corner_s,
    copies, basis_ext, powers, side_ext, fields_ext, faces, start_powers,
):
    del basis_in, powers_in
    rows, cols = mask.shape
    wide = cols + LANES
    tall = rows + 2 * DEPTH
    tiles = cols // LANES
    vectors = basis_ext.shape[1] // tall
    halo_e = jnp.concatenate([corner_n[:DEPTH, :], corner_s[rows - DEPTH : rows, :]], axis=0)
    halo_w = [corner_n[rows : rows + DEPTH, :], corner_s[2 * rows - DEPTH :, :]]
    halo_w = jnp.concatenate(halo_w, axis=0)
    strip_e = jnp.concatenate([from_e[...], halo_e], axis=0)
    strip_w = jnp.concatenate([from_w[...], halo_w], axis=0)

    for k in range(vectors):
        at, to = DEPTH * k, tall * k + rows
        for tile in range(tiles):
            part = pl.ds(tile * LANES, LANES)
            both = [from_n[pl.ds(at, DEPTH), part], from_s[pl.ds(at, DEPTH), part]]
            basis_ext[tile, pl.ds(to, 2 * DEPTH), :] = jnp.concatenate(both, axis=0)
        basis_ext[tiles, pl.ds(to, 2 * DEPTH), :] = edges(k, halo_e, halo_w)
    own = (sides.at[0], sides.at[1], mask, sides.at[2], sides.at[3], sides.at[4])
    for f, ref in enumerate(own):
        at = DEPTH * (vectors + f)
        fields_ext[f, :rows, :cols] = ref[...].astype(jnp.float32)
        fields_ext[f, rows : rows + DEPTH, :cols] = from_n[pl.ds(at, DEPTH), :]
        fields_ext[f, rows + DEPTH :, :cols] = from_s[pl.ds(at, DEPTH), :]
        fields_ext[f, :, cols:] = edges(vectors + f, strip_e, strip_w)
    row = lax.broadcasted_iota(jnp.int32, (tall, wide), 0)
    beyond_n = (row >= rows) & (row < rows + DEPTH) & (place[0] == place[1] - 1)
    beyond_s = (row >= rows + DEPTH) & (place[0] == 0)
    wet = jnp.where(beyond_n | beyond_s, 0.0, fields_ext[2])
    for c, values in enumerate(faces_of(wet, fields_ext[3], fields_ext[4], fields_ext[5])):
        side_ext[c] = values

    for q in range(tall):
        ring_row = (q - DEPTH) % tall
        if q <= 2 * DEPTH or q >= rows - 2:
            spread_faces(side_ext, faces, q, ring_row)
        if ring_row >= rows:
            for tile in range(tiles + 1):
                part = basis_ext[tile, pl.ds(ring_row, vectors, stride=tall), :]
                powers[q, :vectors, tile * LANES : (tile + 1) * LANES] = part
    whole = [side_ext[c] for c in range(5)]
    start = fields_ext[1] - apply_faces(fields_ext[0], whole)
    side_ext[5] = start
    keep_start_powers(start, whole, rows, start_powers)
    for power in range(DEPTH):
        for u in range(DEPTH):
            power_rows(powers, faces, power, 1 + power + u, vectors)
            power_rows(powers, faces, power, tall - 2 - power - u, vectors)
    ends = [range(DEPTH), range(rows - DEPTH, rows)]
    high_sum, cross_sum = products(powers, start_powers, ends, rows)
    high_sum += sums[0]
    cross_sum += sums[1]
    base = (ITERS + 2) * vectors
    count = base + 8
    full = high_sum + cross_sum + cross_sum.T
    full = jnp.concatenate([full, jnp.zeros((count, LANES - count), jnp.float32)], axis=1)
    at = lax.broadcasted_iota(jnp.int32, (vectors, LANES), 1)
    slabs = [full[a * vectors : (a + 1) * vectors, :] for a in range(4)]
    tail = jnp.concatenate([full[base:, :], jnp.zeros((vectors - 8, LANES), jnp.float32)], axis=0)
    out = jnp.zeros((vectors, LANES), jnp.float32)

    def move(out, v, first, width, target):
        moved = pltpu.roll(v, (target - first) % LANES, 1)
        return jnp.where((at >= target) & (at < target + width), moved, out)

    out = move(out, slabs[0], vectors, vectors, 0)
    out = move(out, slabs[1], vectors, 2 * vectors, vectors)
    out = move(out, slabs[2], 2 * vectors, 2 * vectors, 3 * vectors)
    out = move(out, slabs[3], 3 * vectors, 2 * vectors, 5 * vectors)
    free = 7 * vectors
    out = move(out, slabs[0], base, 1, free)
    out = move(out, slabs[1], base, 2, free + 1)
    out = move(out, slabs[2], base + 1, 2, free + 3)
    out = move(out, slabs[3], base + 2, 2, free + 5)
    out = move(out, tail, base, 4, free + 8)

    def one_copy(device, carry):
        copies[device] = out
        return carry

    lax.fori_loop(0, copies.shape[0], one_copy, 0, unroll=8)


def finish_kernel(parts, sides, basis_ext, side_ext, solution, residual, spread):
    _, tall, wide = side_ext.shape
    _, rows, cols = sides.shape
    vectors = basis_ext.shape[1] // tall
    free = 7 * vectors
    several = 8

    def add_parts(i, sums):
        return tuple(sums[n] + parts[i * several + n] for n in range(several))

    nothing = (jnp.zeros(parts.shape[1:], jnp.float32),) * several
    sums = list(lax.fori_loop(0, parts.shape[0] // several, add_parts, nothing, unroll=2))
    while len(sums) > 1:
        sums = [sums[i] + sums[i + 1] for i in range(0, len(sums), 2)]
    total = sums[0]
    lane = lax.broadcasted_iota(jnp.int32, (vectors, LANES), 1)
    sub = lax.broadcasted_iota(jnp.int32, (vectors, LANES), 0)
    table = total
    for i in range(vectors):
        column = table[:, i : i + 1]
        pivot_row = table[i : i + 1, :] / table[i : i + 1, i : i + 1]
        table = jnp.where(sub == i, pivot_row, table - column * pivot_row)
    own_lane = (lane % vectors) == sub
    z = [-table[:, free : free + 1]]
    sums = jnp.zeros((vectors, LANES), jnp.float32)
    history = jnp.zeros((1, LANES), jnp.float32)
    lane_row = lane[:1, :]
    for j in range(2 * ITERS):
        newest = jnp.sum(jnp.where(own_lane, z[j], 0.0), axis=0, keepdims=True)
        history = pltpu.roll(history, vectors, 1)
        history = jnp.where((lane_row >= vectors) & (lane_row < 2 * vectors), newest, history)
        terms = (lane >= vectors) & (lane < (j + 2) * vectors)
        weights = jnp.where(terms, history, jnp.where(lane == free + 1 + j, 1.0, 0.0))
        z.append(-jnp.sum(table * weights, axis=1, keepdims=True))
    for j in range(2 * ITERS + 1):
        sums = sums + pltpu.roll(jnp.where(lane >= free, total, 0.0) * z[j], j, 1)
    picked = jnp.where((lane > free) & (lane < free + 7), sums, 0.0)
    for a in range(ITERS):
        moved = pltpu.roll(total, (a - 7) % LANES, 1)
        first = free + 1 + 2 * a
        picked += jnp.where((sub == a) & (lane >= first) & (lane < first + 2), moved, 0.0)
    moment_row = jnp.sum(picked, axis=0, keepdims=True)
    mu = [moment_row[:, free + 1 + k : free + 2 + k] for k in range(2 * ITERS)]
    for i in range(ITERS + 1):
        spread[i] = jnp.broadcast_to(z[i], (vectors, LANES))

    nil = jnp.zeros((1, 1), jnp.float32)
    rho = [nil + 1.0] + [nil] * ITERS
    gamma = [nil] * (ITERS + 1)
    delta = [nil] * ITERS
    curv = nil
    prev = nil
    for j in range(ITERS):
        norm = nil
        image = nil
        for a in range(j + 1):
            for b in range(j + 1):
                pair = rho[a] * rho[b]
                norm += pair * mu[a + b]
                image += pair * (mu[a + b + 1] + SHIFT * mu[a + b])
        if j == 0:
            gamma = list(rho)
            curv = image
        else:
            ratio = norm / prev
            gamma = [rho[i] + ratio * gamma[i] for i in range(ITERS + 1)]
            curv = image - ratio * ratio * curv
        step = norm / curv
        delta = [delta[i] + step * gamma[i] for i in range(ITERS)]
        below = [nil] + gamma[:ITERS]
        rho = [rho[i] - step * (SHIFT * gamma[i] + below[i]) for i in range(ITERS + 1)]
        prev = norm

    along = [[] for _ in range(ITERS + 1)]
    for tile in range(wide // LANES):
        acc = [jnp.zeros((tall, LANES), jnp.float32) for _ in range(ITERS + 1)]
        for k in range(vectors):
            w = basis_ext[tile, pl.ds(tall * k, tall), :]
            for i in range(ITERS + 1):
                acc[i] = acc[i] + w * spread[i, pl.ds(k, 1), :]
        for i in range(ITERS + 1):
            along[i].append(acc[i])
    along = [jnp.concatenate(pieces, axis=1) for pieces in along]
    faces = [side_ext[c] for c in range(5)]
    v = side_ext[5] + apply_faces(along[0], faces)
    x = sides[0] - along[0][:rows, :cols]
    r = rho[0] * v[:rows, :cols]
    for i in range(ITERS):
        x = x + delta[i] * (v + along[i + 1])[:rows, :cols]
        v = apply_faces(v, faces, SHIFT) + apply_faces(along[i + 1], faces)
        r = r + rho[i + 1] * v[:rows, :cols]
    solution[...] = x
    residual[...] = r


def call(kernel, out_shape, spaces, inputs, scratch=(), name=None, flops=10**6, aliases={}):
    return pl.pallas_call(
        kernel,
        out_shape=out_shape,
        in_specs=[pl.BlockSpec(memory_space=space) for space in spaces],
        out_specs=[pl.BlockSpec(memory_space=pltpu.VMEM)] * len(out_shape),
        scratch_shapes=scratch,
        name=name,
        input_output_aliases=aliases,
        cost_estimate=pl.CostEstimate(flops=flops, bytes_accessed=10**6, transcendentals=0),
        compiler_params=pltpu.CompilerParams(vmem_limit_bytes=24 * 1024 * 1024),
    )(*inputs)


def f32(*shape):
    return jax.ShapeDtypeStruct(shape, jnp.float32)


def shards(right_side, first_guess, cell_mask, cond_east, cond_north, surface, recycled):
    vectors, rows, cols = recycled.shape
    n_lat, n_lon = lax.axis_size("lat"), lax.axis_size("lon")
    devices = n_lat * n_lon
    fields = vectors + 6
    tall, wide = rows + 2 * DEPTH, cols + LANES
    tiles = cols // LANES
    own = (recycled, first_guess, right_side, cell_mask, cond_east, cond_north, surface)
    band, strip = f32(fields * DEPTH, cols), f32(rows, LANES)
    basis, sides, mask, to_n, to_s, to_e, to_w = call(
        pack_kernel,
        [f32(vectors, rows, cols), f32(5, rows, cols), jax.ShapeDtypeStruct((rows, cols), jnp.int32)]
        + [band, band, strip, strip],
        [pltpu.HBM] * 7,
        [pltpu.with_memory_space_constraint(array, pltpu.HBM) for array in own],
        scratch=[pltpu.SemaphoreType.DMA((7,))],
        name="pack",
    )
    north, south = ring(n_lat, 1), ring(n_lat, -1)
    from_w = lax.ppermute(to_e, "lon", ring(n_lon, 1))
    from_e = lax.ppermute(to_w, "lon", ring(n_lon, -1))
    from_s = lax.ppermute(to_n, "lat", north)
    from_n = lax.ppermute(to_s, "lat", south)
    strips = jnp.concatenate([from_e, from_w], axis=0)
    corner_s = lax.ppermute(strips, "lat", north)
    corner_n = lax.ppermute(strips, "lat", south)
    place = jnp.stack([lax.axis_index("lat"), jnp.int32(n_lat)])
    count = (ITERS + 2) * vectors
    powers = f32(tall, count, wide)
    basis_ext = f32(tiles + 1, vectors * tall, LANES)
    faces = pltpu.VMEM((5, tall, 8, wide), jnp.float32)
    start_powers = pltpu.VMEM((tiles, 8 * rows, LANES), jnp.float32)
    powers, basis_ext, sums = call(
        inner_kernel,
        [powers, basis_ext, f32(2, count + 8, count + 8)],
        [pltpu.VMEM] * 5,
        (basis, sides, mask, from_e, from_w),
        scratch=[pltpu.VMEM((5, rows, wide), jnp.float32), faces, start_powers],
        name="inner",
        flops=10**9,
    )
    copies, basis_ext, _, side_ext = call(
        outer_kernel,
        [f32(devices, vectors, LANES), basis_ext, powers, f32(6, tall, wide)],
        [pltpu.SMEM] + [pltpu.VMEM] * 11,
        (place, basis_ext, powers, sums, sides, mask)
        + (from_n, from_s, from_e, from_w, corner_n, corner_s),
        scratch=[pltpu.VMEM((6, tall, wide), jnp.float32), faces, start_powers],
        name="outer",
        aliases={1: 1, 2: 2},
    )
    parts = lax.all_to_all(copies, ("lat", "lon"), 0, 0)
    return call(
        finish_kernel,
        [f32(rows, cols), f32(rows, cols)],
        [pltpu.VMEM] * 4,
        (parts, sides, basis_ext, side_ext),
        scratch=[pltpu.VMEM((ITERS + 1, vectors, LANES), jnp.float32)],
        name="finish",
    )


def solution(mesh):
    block = P("lat", "lon")
    return jax.shard_map(
        shards,
        mesh=mesh,
        in_specs=(block,) * 6 + (P(None, "lat", "lon"),),
        out_specs=(block, block),
        check_vma=False,
    )
```

```python
import jax
import jax.numpy as jnp
from jax import lax
from jax.experimental import pallas as pl
from jax.experimental.pallas import tpu as pltpu
from jax.sharding import PartitionSpec as P

SHIFT = 5.0
ITERS = 3
DEPTH = ITERS + 1
LANES = 128


def ring(count, step):
    return [(i, (i + step) % count) for i in range(count)]


def pack_kernel(
    basis_hbm, guess_hbm, rhs_hbm, mask_hbm, east_hbm, north_hbm, surf_hbm,
    basis, sides, mask, to_n, to_s, to_e, to_w, sems,
):
    vectors, rows, cols = basis.shape
    moves = [(basis_hbm, basis), (mask_hbm, mask)]
    sources = (guess_hbm, rhs_hbm, east_hbm, north_hbm, surf_hbm)
    moves += [(source, sides.at[i]) for i, source in enumerate(sources)]
    copies = [pltpu.make_async_copy(a, b, sems.at[i]) for i, (a, b) in enumerate(moves)]
    for copy in copies:
        copy.start()
    for copy in copies:
        copy.wait()
    fields = [basis.at[k] for k in range(vectors)]
    fields += [sides.at[0], sides.at[1], mask, sides.at[2], sides.at[3], sides.at[4]]
    strip_e = jnp.zeros((rows, LANES), jnp.float32)
    strip_w = jnp.zeros((rows, LANES), jnp.float32)
    lane = lax.broadcasted_iota(jnp.int32, (rows, LANES), 1)
    for f, ref in enumerate(fields):
        at = DEPTH * f
        to_n[pl.ds(at, DEPTH), :] = ref[rows - DEPTH :, :].astype(jnp.float32)
        to_s[pl.ds(at, DEPTH), :] = ref[:DEPTH, :].astype(jnp.float32)
        here = (lane >= at) & (lane < at + DEPTH)
        last = ref[:, cols - LANES :].astype(jnp.float32)
        first = ref[:, :LANES].astype(jnp.float32)
        strip_e = jnp.where(here, pltpu.roll(last, (at + DEPTH) % LANES, 1), strip_e)
        strip_w = jnp.where(here, pltpu.roll(first, at, 1), strip_w)
    to_e[...] = strip_e
    to_w[...] = strip_w


def roll_lanes(v, by):
    return pltpu.roll(v, by % v.shape[1], 1)


def roll_rows(v, by):
    return pltpu.roll(v, by % v.shape[0], 0)


def apply_faces(v, faces, shift=0.0):
    centre, k_east, k_west, k_north, k_south = faces
    beside = k_east * roll_lanes(v, -1) + k_west * roll_lanes(v, 1)
    above = k_north * roll_rows(v, -1) + k_south * roll_rows(v, 1)
    return (centre - shift) * v - (beside + above)


def edges(f, strip_e, strip_w):
    at = DEPTH * f
    lane = lax.broadcasted_iota(jnp.int32, strip_e.shape, 1)
    edge_e = pltpu.roll(strip_e, (-at) % LANES, 1)
    edge_w = pltpu.roll(strip_w, (LANES - DEPTH - at) % LANES, 1)
    return jnp.where(lane < DEPTH, edge_e, jnp.where(lane >= LANES - DEPTH, edge_w, 0.0))


def faces_of(wet, east, north, surf):
    k_east = east * wet * roll_lanes(wet, -1)
    k_north = north * wet * roll_rows(wet, -1)
    k_west = roll_lanes(k_east, 1)
    k_south = roll_rows(k_north, 1)
    centre = surf * wet + k_east + k_west + k_north + k_south + (1.0 - wet)
    return centre, k_east, k_west, k_north, k_south


def spread_faces(side, faces, q, row):
    for c in range(4):
        line = side[c, row : row + 1, :]
        spread = jnp.broadcast_to(line, (8, line.shape[1]))
        faces[c, q] = spread
        if c == 0:
            faces[4, q] = spread - SHIFT


def power_rows(powers, faces, power, q, vectors):
    source = slice(power * vectors, (power + 1) * vectors)
    target = slice((power + 1) * vectors, (power + 2) * vectors)

    def coefficient(c, q):
        return jnp.concatenate([faces[c, q]] * (vectors // 8), axis=0)

    v = powers[q, source, :]
    beside = coefficient(1, q) * roll_lanes(v, -1) + coefficient(2, q) * roll_lanes(v, 1)
    above = coefficient(3, q) * powers[q + 1, source, :]
    above += coefficient(3, q - 1) * powers[q - 1, source, :]
    middle = coefficient(0 if power == 0 else 4, q)
    powers[q, target, :] = middle * v - (beside + above)


def keep_start_powers(v, faces, rows, start_powers):
    tiles = start_powers.shape[0]
    for power in range(ITERS + 1):
        for tile in range(tiles):
            part = v[:rows, tile * LANES : (tile + 1) * LANES]
            start_powers[tile, pl.ds(power * rows, rows), :] = part
        if power < ITERS:
            v = apply_faces(v, faces, SHIFT)
    spare = (8 - (ITERS + 1)) * rows
    start_powers[:, pl.ds((ITERS + 1) * rows, spare), :] = jnp.zeros(
        (tiles, spare, LANES), jnp.float32
    )


def products(powers, start_powers, batches, rows):
    tiles = start_powers.shape[0]
    nt = (((1,), (1,)), ((), ()))
    high_sum = 0.0
    cross_sum = 0.0
    for batch in batches:
        x = []
        for r in batch:
            tail = [start_powers[t, pl.ds(r, 8, stride=rows), :] for t in range(tiles)]
            tail = jnp.concatenate(tail, axis=1)
            x.append(jnp.concatenate([powers[r + DEPTH, :, : tiles * LANES], tail], axis=0))
        x = jnp.concatenate(x, axis=1)
        high = x.astype(jnp.bfloat16)
        low = (x - high.astype(jnp.float32)).astype(jnp.bfloat16)
        high_sum += lax.dot_general(high, high, nt, preferred_element_type=jnp.float32)
        cross_sum += lax.dot_general(high, low, nt, preferred_element_type=jnp.float32)
    return high_sum, cross_sum


def inner_kernel(
    basis, sides, mask, from_e, from_w,
    powers, basis_ext, sums, side, faces, start_powers,
):
    vectors, rows, cols = basis.shape
    tall = rows + 2 * DEPTH
    tiles = cols // LANES
    strip_e, strip_w = from_e[...], from_w[...]
    for k in range(vectors):
        for tile in range(tiles):
            basis_ext[tile, pl.ds(tall * k, rows), :] = basis[k, :, tile * LANES : (tile + 1) * LANES]
        basis_ext[tiles, pl.ds(tall * k, rows), :] = edges(k, strip_e, strip_w)
    own = (sides[0], sides[1], mask[...].astype(jnp.float32), sides[2], sides[3], sides[4])
    guess, rhs, wet, east, north, surf = [
        jnp.concatenate([v, edges(vectors + f, strip_e, strip_w)], axis=1)
        for f, v in enumerate(own)
    ]
    for c, values in enumerate(faces_of(wet, east, north, surf)):
        side[c] = values
    for row in range(rows):
        spread_faces(side, faces, row + DEPTH, row)
        for tile in range(tiles + 1):
            part = basis_ext[tile, pl.ds(row, vectors, stride=tall), :]
            powers[row + DEPTH, :vectors, tile * LANES : (tile + 1) * LANES] = part
    whole = [side[c] for c in range(5)]
    keep_start_powers(rhs - apply_faces(guess, whole), whole, rows, start_powers)
    for power in range(DEPTH):
        first, last = DEPTH + 1 + power, DEPTH + rows - 1 - power
        unroll = (last - first) // (2 if power < 2 else 1)

        def some_rows(i, carry, power=power, first=first, unroll=unroll):
            for u in range(unroll):
                power_rows(powers, faces, power, first + i * unroll + u, vectors)
            return carry

        lax.fori_loop(0, (last - first) // unroll, some_rows, 0)
    middle = range(DEPTH, rows - DEPTH)
    batches = [middle[at : at + DEPTH] for at in range(0, len(middle), DEPTH)]
    high_sum, cross_sum = products(powers, start_powers, batches, rows)
    sums[0] = high_sum
    sums[1] = cross_sum


def outer_kernel(
    inside, basis_in, powers_in, sums, sides, mask,
    from_n, from_s, from_e, from_w, corner_n, corner_s,
    copies, basis_ext, powers, side_ext, fields_ext, faces, start_powers,
):
    del basis_in, powers_in
    rows, cols = mask.shape
    wide = cols + LANES
    tall = rows + 2 * DEPTH
    tiles = cols // LANES
    vectors = basis_ext.shape[1] // tall
    halo_e = jnp.concatenate([corner_n[:DEPTH, :], corner_s[rows - DEPTH : rows, :]], axis=0)
    halo_w = [corner_n[rows : rows + DEPTH, :], corner_s[2 * rows - DEPTH :, :]]
    halo_w = jnp.concatenate(halo_w, axis=0)
    strip_e = jnp.concatenate([from_e[...], halo_e], axis=0)
    strip_w = jnp.concatenate([from_w[...], halo_w], axis=0)

    for k in range(vectors):
        at, to = DEPTH * k, tall * k + rows
        for tile in range(tiles):
            part = pl.ds(tile * LANES, LANES)
            both = [from_n[pl.ds(at, DEPTH), part], from_s[pl.ds(at, DEPTH), part]]
            basis_ext[tile, pl.ds(to, 2 * DEPTH), :] = jnp.concatenate(both, axis=0)
        basis_ext[tiles, pl.ds(to, 2 * DEPTH), :] = edges(k, halo_e, halo_w)
    own = (sides.at[0], sides.at[1], mask, sides.at[2], sides.at[3], sides.at[4])
    for f, ref in enumerate(own):
        at = DEPTH * (vectors + f)
        fields_ext[f, :rows, :cols] = ref[...].astype(jnp.float32)
        fields_ext[f, rows : rows + DEPTH, :cols] = from_n[pl.ds(at, DEPTH), :]
        fields_ext[f, rows + DEPTH :, :cols] = from_s[pl.ds(at, DEPTH), :]
        fields_ext[f, :, cols:] = edges(vectors + f, strip_e, strip_w)
    wet_halo = fields_ext[2, rows:, :] * jnp.concatenate([inside[...]] * (wide // LANES), axis=1)
    wet = jnp.concatenate([fields_ext[2, :rows, :], wet_halo], axis=0)
    for c, values in enumerate(faces_of(wet, fields_ext[3], fields_ext[4], fields_ext[5])):
        side_ext[c] = values

    for q in range(tall):
        ring_row = (q - DEPTH) % tall
        if q <= 2 * DEPTH or q >= rows - 2:
            spread_faces(side_ext, faces, q, ring_row)
        if ring_row >= rows:
            for tile in range(tiles + 1):
                part = basis_ext[tile, pl.ds(ring_row, vectors, stride=tall), :]
                powers[q, :vectors, tile * LANES : (tile + 1) * LANES] = part
    whole = [side_ext[c] for c in range(5)]
    start = fields_ext[1] - apply_faces(fields_ext[0], whole)
    side_ext[5] = start
    keep_start_powers(start, whole, rows, start_powers)
    for power in range(DEPTH):
        for u in range(DEPTH):
            power_rows(powers, faces, power, 1 + power + u, vectors)
            power_rows(powers, faces, power, tall - 2 - power - u, vectors)
    ends = [range(DEPTH), range(rows - DEPTH, rows)]
    high_sum, cross_sum = products(powers, start_powers, ends, rows)
    high_sum += sums[0]
    cross_sum += sums[1]
    base = (ITERS + 2) * vectors
    count = base + 8
    full = high_sum + cross_sum + cross_sum.T
    full = jnp.concatenate([full, jnp.zeros((count, LANES - count), jnp.float32)], axis=1)
    at = lax.broadcasted_iota(jnp.int32, (vectors, LANES), 1)
    slabs = [full[a * vectors : (a + 1) * vectors, :] for a in range(4)]
    tail = jnp.concatenate([full[base:, :], jnp.zeros((vectors - 8, LANES), jnp.float32)], axis=0)
    out = jnp.zeros((vectors, LANES), jnp.float32)

    def move(out, v, first, width, target):
        moved = pltpu.roll(v, (target - first) % LANES, 1)
        return jnp.where((at >= target) & (at < target + width), moved, out)

    out = move(out, slabs[0], vectors, vectors, 0)
    out = move(out, slabs[1], vectors, 2 * vectors, vectors)
    out = move(out, slabs[2], 2 * vectors, 2 * vectors, 3 * vectors)
    out = move(out, slabs[3], 3 * vectors, 2 * vectors, 5 * vectors)
    free = 7 * vectors
    out = move(out, slabs[0], base, 1, free)
    out = move(out, slabs[1], base, 2, free + 1)
    out = move(out, slabs[2], base + 1, 2, free + 3)
    out = move(out, slabs[3], base + 2, 2, free + 5)
    out = move(out, tail, base, 4, free + 8)

    def one_copy(device, carry):
        copies[device] = out
        return carry

    lax.fori_loop(0, copies.shape[0], one_copy, 0, unroll=8)


def finish_kernel(parts, sides, basis_ext, side_ext, solution, residual, spread):
    _, tall, wide = side_ext.shape
    _, rows, cols = sides.shape
    vectors = basis_ext.shape[1] // tall
    free = 7 * vectors
    several = 8

    def add_parts(i, sums):
        return tuple(sums[n] + parts[i * several + n] for n in range(several))

    nothing = (jnp.zeros(parts.shape[1:], jnp.float32),) * several
    sums = list(lax.fori_loop(0, parts.shape[0] // several, add_parts, nothing, unroll=2))
    while len(sums) > 1:
        sums = [sums[i] + sums[i + 1] for i in range(0, len(sums), 2)]
    total = sums[0]
    lane = lax.broadcasted_iota(jnp.int32, (vectors, LANES), 1)
    sub = lax.broadcasted_iota(jnp.int32, (vectors, LANES), 0)
    table = total
    for i in range(vectors):
        column = table[:, i : i + 1]
        pivot_row = table[i : i + 1, :] / table[i : i + 1, i : i + 1]
        table = jnp.where(sub == i, pivot_row, table - column * pivot_row)
    own_lane = (lane % vectors) == sub
    z = [-table[:, free : free + 1]]
    sums = jnp.zeros((vectors, LANES), jnp.float32)
    history = jnp.zeros((1, LANES), jnp.float32)
    lane_row = lane[:1, :]
    for j in range(2 * ITERS):
        newest = jnp.sum(jnp.where(own_lane, z[j], 0.0), axis=0, keepdims=True)
        history = pltpu.roll(history, vectors, 1)
        history = jnp.where((lane_row >= vectors) & (lane_row < 2 * vectors), newest, history)
        terms = (lane >= vectors) & (lane < (j + 2) * vectors)
        weights = jnp.where(terms, history, jnp.where(lane == free + 1 + j, 1.0, 0.0))
        z.append(-jnp.sum(table * weights, axis=1, keepdims=True))
    for j in range(2 * ITERS + 1):
        sums = sums + pltpu.roll(jnp.where(lane >= free, total, 0.0) * z[j], j, 1)
    picked = jnp.where((lane > free) & (lane < free + 7), sums, 0.0)
    for a in range(ITERS):
        moved = pltpu.roll(total, (a - 7) % LANES, 1)
        first = free + 1 + 2 * a
        picked += jnp.where((sub == a) & (lane >= first) & (lane < first + 2), moved, 0.0)
    moment_row = jnp.sum(picked, axis=0, keepdims=True)
    mu = [moment_row[:, free + 1 + k : free + 2 + k] for k in range(2 * ITERS)]
    for i in range(ITERS + 1):
        spread[i] = jnp.broadcast_to(z[i], (vectors, LANES))

    nil = jnp.zeros((1, 1), jnp.float32)
    rho = [nil + 1.0] + [nil] * ITERS
    gamma = [nil] * (ITERS + 1)
    delta = [nil] * ITERS
    curv = nil
    prev = nil
    for j in range(ITERS):
        norm = nil
        image = nil
        for a in range(j + 1):
            for b in range(j + 1):
                pair = rho[a] * rho[b]
                norm += pair * mu[a + b]
                image += pair * (mu[a + b + 1] + SHIFT * mu[a + b])
        if j == 0:
            gamma = list(rho)
            curv = image
        else:
            ratio = norm / prev
            gamma = [rho[i] + ratio * gamma[i] for i in range(ITERS + 1)]
            curv = image - ratio * ratio * curv
        step = norm / curv
        delta = [delta[i] + step * gamma[i] for i in range(ITERS)]
        below = [nil] + gamma[:ITERS]
        rho = [rho[i] - step * (SHIFT * gamma[i] + below[i]) for i in range(ITERS + 1)]
        prev = norm

    along = [[] for _ in range(ITERS + 1)]
    for tile in range(wide // LANES):
        acc = [jnp.zeros((tall, LANES), jnp.float32) for _ in range(ITERS + 1)]
        for k in range(vectors):
            w = basis_ext[tile, pl.ds(tall * k, tall), :]
            for i in range(ITERS + 1):
                acc[i] = acc[i] + w * spread[i, pl.ds(k, 1), :]
        for i in range(ITERS + 1):
            along[i].append(acc[i])
    along = [jnp.concatenate(pieces, axis=1) for pieces in along]
    faces = [side_ext[c] for c in range(5)]
    v = side_ext[5] + apply_faces(along[0], faces)
    x = sides[0] - along[0][:rows, :cols]
    r = rho[0] * v[:rows, :cols]
    for i in range(ITERS):
        x = x + delta[i] * (v + along[i + 1])[:rows, :cols]
        v = apply_faces(v, faces, SHIFT) + apply_faces(along[i + 1], faces)
        r = r + rho[i + 1] * v[:rows, :cols]
    solution[...] = x
    residual[...] = r


def call(kernel, out_shape, spaces, inputs, scratch=(), flops=10**6, aliases={}):
    return pl.pallas_call(
        kernel,
        out_shape=out_shape,
        in_specs=[pl.BlockSpec(memory_space=space) for space in spaces],
        out_specs=[pl.BlockSpec(memory_space=pltpu.VMEM)] * len(out_shape),
        scratch_shapes=scratch,
        input_output_aliases=aliases,
        cost_estimate=pl.CostEstimate(flops=flops, bytes_accessed=10**6, transcendentals=0),
        compiler_params=pltpu.CompilerParams(vmem_limit_bytes=24 * 1024 * 1024),
    )(*inputs)


def f32(*shape):
    return jax.ShapeDtypeStruct(shape, jnp.float32)


def shards(right_side, first_guess, cell_mask, cond_east, cond_north, surface, recycled):
    vectors, rows, cols = recycled.shape
    n_lat, n_lon = lax.axis_size("lat"), lax.axis_size("lon")
    devices = n_lat * n_lon
    fields = vectors + 6
    tall, wide = rows + 2 * DEPTH, cols + LANES
    tiles = cols // LANES
    own = (recycled, first_guess, right_side, cell_mask, cond_east, cond_north, surface)
    band, strip = f32(fields * DEPTH, cols), f32(rows, LANES)
    basis, sides, mask, to_n, to_s, to_e, to_w = call(
        pack_kernel,
        [f32(vectors, rows, cols), f32(5, rows, cols), jax.ShapeDtypeStruct((rows, cols), jnp.int32)]
        + [band, band, strip, strip],
        [pltpu.HBM] * 7,
        [pltpu.with_memory_space_constraint(array, pltpu.HBM) for array in own],
        scratch=[pltpu.SemaphoreType.DMA((7,))],
    )
    north, south = ring(n_lat, 1), ring(n_lat, -1)
    from_w = lax.ppermute(to_e, "lon", ring(n_lon, 1))
    from_e = lax.ppermute(to_w, "lon", ring(n_lon, -1))
    from_s = lax.ppermute(to_n, "lat", north)
    from_n = lax.ppermute(to_s, "lat", south)
    strips = jnp.concatenate([from_e, from_w], axis=0)
    corner_s = lax.ppermute(strips, "lat", north)
    corner_n = lax.ppermute(strips, "lat", south)
    here = lax.axis_index("lat")
    inside = jnp.stack([here < n_lat - 1, here > 0]).astype(jnp.float32)
    inside = jnp.broadcast_to(inside[:, None, None], (2, DEPTH, LANES)).reshape(-1, LANES)
    count = (ITERS + 2) * vectors
    powers = f32(tall, count, wide)
    basis_ext = f32(tiles + 1, vectors * tall, LANES)
    faces = pltpu.VMEM((5, tall, 8, wide), jnp.float32)
    start_powers = pltpu.VMEM((tiles, 8 * rows, LANES), jnp.float32)
    powers, basis_ext, sums = call(
        inner_kernel,
        [powers, basis_ext, f32(2, count + 8, count + 8)],
        [pltpu.VMEM] * 5,
        (basis, sides, mask, from_e, from_w),
        scratch=[pltpu.VMEM((5, rows, wide), jnp.float32), faces, start_powers],
        flops=10**9,
    )
    copies, basis_ext, _, side_ext = call(
        outer_kernel,
        [f32(devices, vectors, LANES), basis_ext, powers, f32(6, tall, wide)],
        [pltpu.VMEM] * 12,
        (inside, basis_ext, powers, sums, sides, mask)
        + (from_n, from_s, from_e, from_w, corner_n, corner_s),
        scratch=[pltpu.VMEM((6, tall, wide), jnp.float32), faces, start_powers],
        aliases={1: 1, 2: 2},
    )
    parts = lax.all_to_all(copies, ("lat", "lon"), 0, 0)
    return call(
        finish_kernel,
        [f32(rows, cols), f32(rows, cols)],
        [pltpu.VMEM] * 4,
        (parts, sides, basis_ext, side_ext),
        scratch=[pltpu.VMEM((ITERS + 1, vectors, LANES), jnp.float32)],
    )


def solution(mesh):
    block = P("lat", "lon")
    return jax.shard_map(
        shards,
        mesh=mesh,
        in_specs=(block,) * 6 + (P(None, "lat", "lon"),),
        out_specs=(block, block),
        check_vma=False,
    )
```

```python
import jax
import jax.numpy as jnp
from jax import lax
from jax.experimental import pallas as pl
from jax.experimental.pallas import tpu as pltpu
from jax.sharding import PartitionSpec as P

SHIFT = 5.0
ITERS = 3
DEPTH = ITERS + 1
LANES = 128


def ring(count, step):
    return [(i, (i + step) % count) for i in range(count)]


def pack_kernel(
    basis_hbm, guess_hbm, rhs_hbm, mask_hbm, east_hbm, north_hbm, surf_hbm,
    basis, sides, mask, to_n, to_s, to_e, to_w, sems,
):
    vectors, rows, cols = basis.shape
    moves = [(basis_hbm, basis), (mask_hbm, mask)]
    sources = (guess_hbm, rhs_hbm, east_hbm, north_hbm, surf_hbm)
    moves += [(source, sides.at[i]) for i, source in enumerate(sources)]
    copies = [pltpu.make_async_copy(a, b, sems.at[i]) for i, (a, b) in enumerate(moves)]
    for copy in copies:
        copy.start()
    for copy in copies:
        copy.wait()
    fields = [basis.at[k] for k in range(vectors)]
    fields += [sides.at[0], sides.at[1], mask, sides.at[2], sides.at[3], sides.at[4]]
    strip_e = jnp.zeros((rows, LANES), jnp.float32)
    strip_w = jnp.zeros((rows, LANES), jnp.float32)
    lane = lax.broadcasted_iota(jnp.int32, (rows, LANES), 1)
    for f, ref in enumerate(fields):
        at = DEPTH * f
        to_n[pl.ds(at, DEPTH), :] = ref[rows - DEPTH :, :].astype(jnp.float32)
        to_s[pl.ds(at, DEPTH), :] = ref[:DEPTH, :].astype(jnp.float32)
        here = (lane >= at) & (lane < at + DEPTH)
        last = ref[:, cols - LANES :].astype(jnp.float32)
        first = ref[:, :LANES].astype(jnp.float32)
        strip_e = jnp.where(here, pltpu.roll(last, (at + DEPTH) % LANES, 1), strip_e)
        strip_w = jnp.where(here, pltpu.roll(first, at, 1), strip_w)
    to_e[...] = strip_e
    to_w[...] = strip_w


def roll_lanes(v, by):
    return pltpu.roll(v, by % v.shape[1], 1)


def roll_rows(v, by):
    return pltpu.roll(v, by % v.shape[0], 0)


def apply_faces(v, faces, shift=0.0):
    centre, k_east, k_west, k_north, k_south = faces
    beside = k_east * roll_lanes(v, -1) + k_west * roll_lanes(v, 1)
    above = k_north * roll_rows(v, -1) + k_south * roll_rows(v, 1)
    return (centre - shift) * v - (beside + above)


def edges(f, strip_e, strip_w):
    at = DEPTH * f
    lane = lax.broadcasted_iota(jnp.int32, strip_e.shape, 1)
    edge_e = pltpu.roll(strip_e, (-at) % LANES, 1)
    edge_w = pltpu.roll(strip_w, (LANES - DEPTH - at) % LANES, 1)
    return jnp.where(lane < DEPTH, edge_e, jnp.where(lane >= LANES - DEPTH, edge_w, 0.0))


def faces_of(wet, east, north, surf):
    k_east = east * wet * roll_lanes(wet, -1)
    k_north = north * wet * roll_rows(wet, -1)
    k_west = roll_lanes(k_east, 1)
    k_south = roll_rows(k_north, 1)
    centre = surf * wet + k_east + k_west + k_north + k_south + (1.0 - wet)
    return centre, k_east, k_west, k_north, k_south


def spread_faces(side, faces, q, row):
    for c in range(4):
        line = side[c, row : row + 1, :]
        spread = jnp.broadcast_to(line, (8, line.shape[1]))
        faces[c, q] = spread
        if c == 0:
            faces[4, q] = spread - SHIFT


def power_rows(powers, faces, power, q, vectors):
    source = slice(power * vectors, (power + 1) * vectors)
    target = slice((power + 1) * vectors, (power + 2) * vectors)

    def coefficient(c, q):
        return jnp.concatenate([faces[c, q]] * (vectors // 8), axis=0)

    v = powers[q, source, :]
    beside = coefficient(1, q) * roll_lanes(v, -1) + coefficient(2, q) * roll_lanes(v, 1)
    above = coefficient(3, q) * powers[q + 1, source, :]
    above += coefficient(3, q - 1) * powers[q - 1, source, :]
    middle = coefficient(0 if power == 0 else 4, q)
    powers[q, target, :] = middle * v - (beside + above)


def keep_start_powers(v, faces, rows, start_powers):
    tiles = start_powers.shape[0]
    for power in range(ITERS + 1):
        for tile in range(tiles):
            part = v[:rows, tile * LANES : (tile + 1) * LANES]
            start_powers[tile, pl.ds(power * rows, rows), :] = part
        if power < ITERS:
            v = apply_faces(v, faces, SHIFT)
    spare = (8 - (ITERS + 1)) * rows
    start_powers[:, pl.ds((ITERS + 1) * rows, spare), :] = jnp.zeros(
        (tiles, spare, LANES), jnp.float32
    )


def products(powers, start_powers, batches, rows):
    tiles = start_powers.shape[0]
    nt = (((1,), (1,)), ((), ()))
    total = 0.0
    for batch in batches:
        x = []
        for r in batch:
            tail = [start_powers[t, pl.ds(r, 8, stride=rows), :] for t in range(tiles)]
            tail = jnp.concatenate(tail, axis=1)
            x.append(jnp.concatenate([powers[r + DEPTH, :, : tiles * LANES], tail], axis=0))
        x = jnp.concatenate(x, axis=1)
        high = x.astype(jnp.bfloat16)
        low = (x - high.astype(jnp.float32)).astype(jnp.bfloat16)
        both = jnp.concatenate([high, low], axis=0)
        total += lax.dot_general(both, high, nt, preferred_element_type=jnp.float32)
    return total


def inner_kernel(
    basis, sides, mask, from_e, from_w,
    powers, basis_ext, sums, side, faces, start_powers,
):
    vectors, rows, cols = basis.shape
    tall = rows + 2 * DEPTH
    tiles = cols // LANES
    strip_e, strip_w = from_e[...], from_w[...]
    for k in range(vectors):
        for tile in range(tiles):
            basis_ext[tile, pl.ds(tall * k, rows), :] = basis[k, :, tile * LANES : (tile + 1) * LANES]
        basis_ext[tiles, pl.ds(tall * k, rows), :] = edges(k, strip_e, strip_w)
    own = (sides[0], sides[1], mask[...].astype(jnp.float32), sides[2], sides[3], sides[4])
    guess, rhs, wet, east, north, surf = [
        jnp.concatenate([v, edges(vectors + f, strip_e, strip_w)], axis=1)
        for f, v in enumerate(own)
    ]
    for c, values in enumerate(faces_of(wet, east, north, surf)):
        side[c] = values
    for row in range(rows):
        spread_faces(side, faces, row + DEPTH, row)
        for tile in range(tiles + 1):
            part = basis_ext[tile, pl.ds(row, vectors, stride=tall), :]
            powers[row + DEPTH, :vectors, tile * LANES : (tile + 1) * LANES] = part
    whole = [side[c] for c in range(5)]
    keep_start_powers(rhs - apply_faces(guess, whole), whole, rows, start_powers)
    for power in range(DEPTH):
        first, last = DEPTH + 1 + power, DEPTH + rows - 1 - power
        unroll = (last - first) // (2 if power < 2 else 1)

        def some_rows(i, carry, power=power, first=first, unroll=unroll):
            for u in range(unroll):
                power_rows(powers, faces, power, first + i * unroll + u, vectors)
            return carry

        lax.fori_loop(0, (last - first) // unroll, some_rows, 0)
    middle = range(DEPTH, rows - DEPTH)
    batches = [middle[at : at + DEPTH] for at in range(0, len(middle), DEPTH)]
    sums[...] = products(powers, start_powers, batches, rows)


def outer_kernel(
    inside, basis_in, powers_in, sums, sides, mask,
    from_n, from_s, from_e, from_w, corner_n, corner_s,
    copies, basis_ext, powers, side_ext, fields_ext, faces, start_powers,
):
    del basis_in, powers_in
    rows, cols = mask.shape
    wide = cols + LANES
    tall = rows + 2 * DEPTH
    tiles = cols // LANES
    vectors = basis_ext.shape[1] // tall
    halo_e = jnp.concatenate([corner_n[:DEPTH, :], corner_s[rows - DEPTH : rows, :]], axis=0)
    halo_w = [corner_n[rows : rows + DEPTH, :], corner_s[2 * rows - DEPTH :, :]]
    halo_w = jnp.concatenate(halo_w, axis=0)
    strip_e = jnp.concatenate([from_e[...], halo_e], axis=0)
    strip_w = jnp.concatenate([from_w[...], halo_w], axis=0)

    for k in range(vectors):
        at, to = DEPTH * k, tall * k + rows
        for tile in range(tiles):
            part = pl.ds(tile * LANES, LANES)
            both = [from_n[pl.ds(at, DEPTH), part], from_s[pl.ds(at, DEPTH), part]]
            basis_ext[tile, pl.ds(to, 2 * DEPTH), :] = jnp.concatenate(both, axis=0)
        basis_ext[tiles, pl.ds(to, 2 * DEPTH), :] = edges(k, halo_e, halo_w)
    own = (sides.at[0], sides.at[1], mask, sides.at[2], sides.at[3], sides.at[4])
    for f, ref in enumerate(own):
        at = DEPTH * (vectors + f)
        fields_ext[f, :rows, :cols] = ref[...].astype(jnp.float32)
        fields_ext[f, rows : rows + DEPTH, :cols] = from_n[pl.ds(at, DEPTH), :]
        fields_ext[f, rows + DEPTH :, :cols] = from_s[pl.ds(at, DEPTH), :]
        fields_ext[f, :, cols:] = edges(vectors + f, strip_e, strip_w)
    wet_halo = fields_ext[2, rows:, :] * jnp.concatenate([inside[...]] * (wide // LANES), axis=1)
    wet = jnp.concatenate([fields_ext[2, :rows, :], wet_halo], axis=0)
    for c, values in enumerate(faces_of(wet, fields_ext[3], fields_ext[4], fields_ext[5])):
        side_ext[c] = values

    for q in range(tall):
        ring_row = (q - DEPTH) % tall
        if q <= 2 * DEPTH or q >= rows - 2:
            spread_faces(side_ext, faces, q, ring_row)
        if ring_row >= rows:
            for tile in range(tiles + 1):
                part = basis_ext[tile, pl.ds(ring_row, vectors, stride=tall), :]
                powers[q, :vectors, tile * LANES : (tile + 1) * LANES] = part
    whole = [side_ext[c] for c in range(5)]
    start = fields_ext[1] - apply_faces(fields_ext[0], whole)
    side_ext[5] = start
    keep_start_powers(start, whole, rows, start_powers)
    for power in range(DEPTH):
        for u in range(DEPTH):
            power_rows(powers, faces, power, 1 + power + u, vectors)
            power_rows(powers, faces, power, tall - 2 - power - u, vectors)
    ends = [range(DEPTH), range(rows - DEPTH, rows)]
    both = products(powers, start_powers, ends, rows) + sums[...]
    base = (ITERS + 2) * vectors
    count = base + 8
    full = both[:count] + both[count:] + both[count:].T
    full = jnp.concatenate([full, jnp.zeros((count, LANES - count), jnp.float32)], axis=1)
    at = lax.broadcasted_iota(jnp.int32, (vectors, LANES), 1)
    slabs = [full[a * vectors : (a + 1) * vectors, :] for a in range(4)]
    tail = jnp.concatenate([full[base:, :], jnp.zeros((vectors - 8, LANES), jnp.float32)], axis=0)
    out = jnp.zeros((vectors, LANES), jnp.float32)

    def move(out, v, first, width, target):
        moved = pltpu.roll(v, (target - first) % LANES, 1)
        return jnp.where((at >= target) & (at < target + width), moved, out)

    out = move(out, slabs[0], vectors, vectors, 0)
    out = move(out, slabs[1], vectors, 2 * vectors, vectors)
    out = move(out, slabs[2], 2 * vectors, 2 * vectors, 3 * vectors)
    out = move(out, slabs[3], 3 * vectors, 2 * vectors, 5 * vectors)
    free = 7 * vectors
    out = move(out, slabs[0], base, 1, free)
    out = move(out, slabs[1], base, 2, free + 1)
    out = move(out, slabs[2], base + 1, 2, free + 3)
    out = move(out, slabs[3], base + 2, 2, free + 5)
    out = move(out, tail, base, 4, free + 8)

    def one_copy(device, carry):
        copies[device] = out
        return carry

    lax.fori_loop(0, copies.shape[0], one_copy, 0, unroll=8)


def finish_kernel(parts, sides, basis_ext, side_ext, solution, residual, spread):
    _, tall, wide = side_ext.shape
    _, rows, cols = sides.shape
    vectors = basis_ext.shape[1] // tall
    free = 7 * vectors
    several = 8

    def add_parts(i, sums):
        return tuple(sums[n] + parts[i * several + n] for n in range(several))

    nothing = (jnp.zeros(parts.shape[1:], jnp.float32),) * several
    sums = list(lax.fori_loop(0, parts.shape[0] // several, add_parts, nothing, unroll=2))
    while len(sums) > 1:
        sums = [sums[i] + sums[i + 1] for i in range(0, len(sums), 2)]
    total = sums[0]
    lane = lax.broadcasted_iota(jnp.int32, (vectors, LANES), 1)
    sub = lax.broadcasted_iota(jnp.int32, (vectors, LANES), 0)
    table = total
    columns = [jnp.broadcast_to(total[:, i : i + 1], total.shape) for i in range(vectors)]

    def row_of(values, i):
        return jnp.broadcast_to(values[i : i + 1, :], values.shape)

    for i in range(vectors):
        column = columns[i]
        inverse = 1.0 / row_of(column, i)

        def eliminate(values):
            pivot_row = row_of(values, i) * inverse
            return jnp.where(sub == i, pivot_row, values - column * pivot_row)

        columns[i + 1 :] = [eliminate(values) for values in columns[i + 1 :]]
        table = eliminate(table)
    own_lane = (lane % vectors) == sub
    z = [-table[:, free : free + 1]]
    sums = jnp.zeros((vectors, LANES), jnp.float32)
    history = jnp.zeros((1, LANES), jnp.float32)
    lane_row = lane[:1, :]
    for j in range(2 * ITERS):
        newest = jnp.sum(jnp.where(own_lane, z[j], 0.0), axis=0, keepdims=True)
        history = pltpu.roll(history, vectors, 1)
        history = jnp.where((lane_row >= vectors) & (lane_row < 2 * vectors), newest, history)
        terms = (lane >= vectors) & (lane < (j + 2) * vectors)
        weights = jnp.where(terms, history, jnp.where(lane == free + 1 + j, 1.0, 0.0))
        z.append(-jnp.sum(table * weights, axis=1, keepdims=True))
    for j in range(2 * ITERS + 1):
        sums = sums + pltpu.roll(jnp.where(lane >= free, total, 0.0) * z[j], j, 1)
    picked = jnp.where((lane > free) & (lane < free + 7), sums, 0.0)
    for a in range(ITERS):
        moved = pltpu.roll(total, (a - 7) % LANES, 1)
        first = free + 1 + 2 * a
        picked += jnp.where((sub == a) & (lane >= first) & (lane < first + 2), moved, 0.0)
    moment_row = jnp.sum(picked, axis=0, keepdims=True)
    mu = [moment_row[:, free + 1 + k : free + 2 + k] for k in range(2 * ITERS)]
    for i in range(ITERS + 1):
        spread[i] = jnp.broadcast_to(z[i], (vectors, LANES))

    nil = jnp.zeros((1, 1), jnp.float32)
    rho = [nil + 1.0] + [nil] * ITERS
    gamma = [nil] * (ITERS + 1)
    delta = [nil] * ITERS
    curv = nil
    prev = nil
    for j in range(ITERS):
        norm = nil
        image = nil
        for a in range(j + 1):
            for b in range(j + 1):
                pair = rho[a] * rho[b]
                norm += pair * mu[a + b]
                image += pair * (mu[a + b + 1] + SHIFT * mu[a + b])
        if j == 0:
            gamma = list(rho)
            curv = image
        else:
            ratio = norm / prev
            gamma = [rho[i] + ratio * gamma[i] for i in range(ITERS + 1)]
            curv = image - ratio * ratio * curv
        step = norm / curv
        delta = [delta[i] + step * gamma[i] for i in range(ITERS)]
        below = [nil] + gamma[:ITERS]
        rho = [rho[i] - step * (SHIFT * gamma[i] + below[i]) for i in range(ITERS + 1)]
        prev = norm

    along = [[] for _ in range(ITERS + 1)]
    for tile in range(wide // LANES):
        acc = [jnp.zeros((tall, LANES), jnp.float32) for _ in range(ITERS + 1)]
        for k in range(vectors):
            w = basis_ext[tile, pl.ds(tall * k, tall), :]
            for i in range(ITERS + 1):
                acc[i] = acc[i] + w * spread[i, pl.ds(k, 1), :]
        for i in range(ITERS + 1):
            along[i].append(acc[i])
    along = [jnp.concatenate(pieces, axis=1) for pieces in along]
    faces = [side_ext[c] for c in range(5)]
    v = side_ext[5] + apply_faces(along[0], faces)
    x = sides[0] - along[0][:rows, :cols]
    r = rho[0] * v[:rows, :cols]
    for i in range(ITERS):
        x = x + delta[i] * (v + along[i + 1])[:rows, :cols]
        v = apply_faces(v, faces, SHIFT) + apply_faces(along[i + 1], faces)
        r = r + rho[i + 1] * v[:rows, :cols]
    solution[...] = x
    residual[...] = r


def call(kernel, out_shape, spaces, inputs, scratch=(), flops=10**6, aliases={}):
    return pl.pallas_call(
        kernel,
        out_shape=out_shape,
        in_specs=[pl.BlockSpec(memory_space=space) for space in spaces],
        out_specs=[pl.BlockSpec(memory_space=pltpu.VMEM)] * len(out_shape),
        scratch_shapes=scratch,
        input_output_aliases=aliases,
        cost_estimate=pl.CostEstimate(flops=flops, bytes_accessed=10**6, transcendentals=0),
        compiler_params=pltpu.CompilerParams(vmem_limit_bytes=24 * 1024 * 1024),
    )(*inputs)


def f32(*shape):
    return jax.ShapeDtypeStruct(shape, jnp.float32)


def shards(right_side, first_guess, cell_mask, cond_east, cond_north, surface, recycled):
    vectors, rows, cols = recycled.shape
    n_lat, n_lon = lax.axis_size("lat"), lax.axis_size("lon")
    devices = n_lat * n_lon
    fields = vectors + 6
    tall, wide = rows + 2 * DEPTH, cols + LANES
    tiles = cols // LANES
    own = (recycled, first_guess, right_side, cell_mask, cond_east, cond_north, surface)
    band, strip = f32(fields * DEPTH, cols), f32(rows, LANES)
    basis, sides, mask, to_n, to_s, to_e, to_w = call(
        pack_kernel,
        [f32(vectors, rows, cols), f32(5, rows, cols), jax.ShapeDtypeStruct((rows, cols), jnp.int32)]
        + [band, band, strip, strip],
        [pltpu.HBM] * 7,
        [pltpu.with_memory_space_constraint(array, pltpu.HBM) for array in own],
        scratch=[pltpu.SemaphoreType.DMA((7,))],
    )
    north, south = ring(n_lat, 1), ring(n_lat, -1)
    from_w = lax.ppermute(to_e, "lon", ring(n_lon, 1))
    from_e = lax.ppermute(to_w, "lon", ring(n_lon, -1))
    from_s = lax.ppermute(to_n, "lat", north)
    from_n = lax.ppermute(to_s, "lat", south)
    strips = jnp.concatenate([from_e, from_w], axis=0)
    corner_s = lax.ppermute(strips, "lat", north)
    corner_n = lax.ppermute(strips, "lat", south)
    here = lax.axis_index("lat")
    inside = jnp.stack([here < n_lat - 1, here > 0]).astype(jnp.float32)
    inside = jnp.broadcast_to(inside[:, None, None], (2, DEPTH, LANES)).reshape(-1, LANES)
    count = (ITERS + 2) * vectors
    powers = f32(tall, count, wide)
    basis_ext = f32(tiles + 1, vectors * tall, LANES)
    faces = pltpu.VMEM((5, tall, 8, wide), jnp.float32)
    start_powers = pltpu.VMEM((tiles, 8 * rows, LANES), jnp.float32)
    powers, basis_ext, sums = call(
        inner_kernel,
        [powers, basis_ext, f32(2 * (count + 8), count + 8)],
        [pltpu.VMEM] * 5,
        (basis, sides, mask, from_e, from_w),
        scratch=[pltpu.VMEM((5, rows, wide), jnp.float32), faces, start_powers],
        flops=10**9,
    )
    copies, basis_ext, _, side_ext = call(
        outer_kernel,
        [f32(devices, vectors, LANES), basis_ext, powers, f32(6, tall, wide)],
        [pltpu.VMEM] * 12,
        (inside, basis_ext, powers, sums, sides, mask)
        + (from_n, from_s, from_e, from_w, corner_n, corner_s),
        scratch=[pltpu.VMEM((6, tall, wide), jnp.float32), faces, start_powers],
        aliases={1: 1, 2: 2},
    )
    parts = lax.all_to_all(copies, ("lat", "lon"), 0, 0)
    return call(
        finish_kernel,
        [f32(rows, cols), f32(rows, cols)],
        [pltpu.VMEM] * 4,
        (parts, sides, basis_ext, side_ext),
        scratch=[pltpu.VMEM((ITERS + 1, vectors, LANES), jnp.float32)],
    )


def solution(mesh):
    block = P("lat", "lon")
    return jax.shard_map(
        shards,
        mesh=mesh,
        in_specs=(block,) * 6 + (P(None, "lat", "lon"),),
        out_specs=(block, block),
        check_vma=False,
    )
```

```python
import jax
import jax.numpy as jnp
from jax import lax
from jax.experimental import pallas as pl
from jax.experimental.pallas import tpu as pltpu
from jax.sharding import PartitionSpec as P

SHIFT = 5.0
ITERS = 3
DEPTH = ITERS + 1
LANES = 128


def ring(count, step):
    return [(i, (i + step) % count) for i in range(count)]


def pack_kernel(
    basis_hbm, guess_hbm, rhs_hbm, mask_hbm, east_hbm, north_hbm, surf_hbm,
    basis, sides, mask, to_n, to_s, to_e, to_w, sems,
):
    vectors, rows, cols = basis.shape
    moves = [(basis_hbm, basis), (mask_hbm, mask)]
    sources = (guess_hbm, rhs_hbm, east_hbm, north_hbm, surf_hbm)
    moves += [(source, sides.at[i]) for i, source in enumerate(sources)]
    copies = [pltpu.make_async_copy(a, b, sems.at[i]) for i, (a, b) in enumerate(moves)]
    for copy in copies:
        copy.start()
    for copy in copies:
        copy.wait()
    fields = [basis.at[k] for k in range(vectors)]
    fields += [sides.at[0], sides.at[1], mask, sides.at[2], sides.at[3], sides.at[4]]
    strip_e = jnp.zeros((rows, LANES), jnp.float32)
    strip_w = jnp.zeros((rows, LANES), jnp.float32)
    lane = lax.broadcasted_iota(jnp.int32, (rows, LANES), 1)
    for f, ref in enumerate(fields):
        at = DEPTH * f
        to_n[pl.ds(at, DEPTH), :] = ref[rows - DEPTH :, :].astype(jnp.float32)
        to_s[pl.ds(at, DEPTH), :] = ref[:DEPTH, :].astype(jnp.float32)
        here = (lane >= at) & (lane < at + DEPTH)
        last = ref[:, cols - LANES :].astype(jnp.float32)
        first = ref[:, :LANES].astype(jnp.float32)
        strip_e = jnp.where(here, pltpu.roll(last, (at + DEPTH) % LANES, 1), strip_e)
        strip_w = jnp.where(here, pltpu.roll(first, at, 1), strip_w)
    to_e[...] = strip_e
    to_w[...] = strip_w


def roll_lanes(v, by):
    return pltpu.roll(v, by % v.shape[1], 1)


def roll_rows(v, by):
    return pltpu.roll(v, by % v.shape[0], 0)


def apply_faces(v, faces, shift=0.0):
    centre, k_east, k_west, k_north, k_south = faces
    beside = k_east * roll_lanes(v, -1) + k_west * roll_lanes(v, 1)
    above = k_north * roll_rows(v, -1) + k_south * roll_rows(v, 1)
    return (centre - shift) * v - (beside + above)


def edges(f, strip_e, strip_w):
    at = DEPTH * f
    lane = lax.broadcasted_iota(jnp.int32, strip_e.shape, 1)
    edge_e = pltpu.roll(strip_e, (-at) % LANES, 1)
    edge_w = pltpu.roll(strip_w, (LANES - DEPTH - at) % LANES, 1)
    return jnp.where(lane < DEPTH, edge_e, jnp.where(lane >= LANES - DEPTH, edge_w, 0.0))


def faces_of(wet, east, north, surf):
    k_east = east * wet * roll_lanes(wet, -1)
    k_north = north * wet * roll_rows(wet, -1)
    k_west = roll_lanes(k_east, 1)
    k_south = roll_rows(k_north, 1)
    centre = surf * wet + k_east + k_west + k_north + k_south + (1.0 - wet)
    return centre, k_east, k_west, k_north, k_south


def spread_faces(side, faces, q, row):
    for c in range(4):
        line = side[c, row : row + 1, :]
        spread = jnp.broadcast_to(line, (8, line.shape[1]))
        faces[c, q] = spread
        if c == 0:
            faces[4, q] = spread - SHIFT


def power_rows(powers, faces, power, q, vectors):
    source = slice(power * vectors, (power + 1) * vectors)
    target = slice((power + 1) * vectors, (power + 2) * vectors)

    def coefficient(c, q):
        return jnp.concatenate([faces[c, q]] * (vectors // 8), axis=0)

    v = powers[q, source, :]
    beside = coefficient(1, q) * roll_lanes(v, -1) + coefficient(2, q) * roll_lanes(v, 1)
    above = coefficient(3, q) * powers[q + 1, source, :]
    above += coefficient(3, q - 1) * powers[q - 1, source, :]
    middle = coefficient(0 if power == 0 else 4, q)
    powers[q, target, :] = middle * v - (beside + above)


def keep_start_powers(v, faces, rows, start_powers):
    tiles = start_powers.shape[0]
    for power in range(ITERS + 1):
        for tile in range(tiles):
            part = v[:rows, tile * LANES : (tile + 1) * LANES]
            start_powers[tile, pl.ds(power * rows, rows), :] = part
        if power < ITERS:
            v = apply_faces(v, faces, SHIFT)
    spare = (8 - (ITERS + 1)) * rows
    start_powers[:, pl.ds((ITERS + 1) * rows, spare), :] = jnp.zeros(
        (tiles, spare, LANES), jnp.float32
    )


def products(powers, start_powers, batches, rows):
    tiles = start_powers.shape[0]
    nt = (((1,), (1,)), ((), ()))
    total = 0.0
    for batch in batches:
        x = []
        for r in batch:
            tail = [start_powers[t, pl.ds(r, 8, stride=rows), :] for t in range(tiles)]
            tail = jnp.concatenate(tail, axis=1)
            x.append(jnp.concatenate([powers[r + DEPTH, :, : tiles * LANES], tail], axis=0))
        x = jnp.concatenate(x, axis=1)
        high = x.astype(jnp.bfloat16)
        low = (x - high.astype(jnp.float32)).astype(jnp.bfloat16)
        both = jnp.concatenate([high, low], axis=0)
        total += lax.dot_general(both, high, nt, preferred_element_type=jnp.float32)
    return total


def inner_kernel(
    basis, sides, mask, from_e, from_w,
    powers, basis_ext, sums, side, faces, start_powers,
):
    vectors, rows, cols = basis.shape
    tall = rows + 2 * DEPTH
    tiles = cols // LANES
    strip_e, strip_w = from_e[...], from_w[...]
    for k in range(vectors):
        for tile in range(tiles):
            basis_ext[tile, pl.ds(tall * k, rows), :] = basis[k, :, tile * LANES : (tile + 1) * LANES]
        basis_ext[tiles, pl.ds(tall * k, rows), :] = edges(k, strip_e, strip_w)
    own = (sides[0], sides[1], mask[...].astype(jnp.float32), sides[2], sides[3], sides[4])
    guess, rhs, wet, east, north, surf = [
        jnp.concatenate([v, edges(vectors + f, strip_e, strip_w)], axis=1)
        for f, v in enumerate(own)
    ]
    for c, values in enumerate(faces_of(wet, east, north, surf)):
        side[c] = values
    for row in range(rows):
        spread_faces(side, faces, row + DEPTH, row)
        for tile in range(tiles + 1):
            part = basis_ext[tile, pl.ds(row, vectors, stride=tall), :]
            powers[row + DEPTH, :vectors, tile * LANES : (tile + 1) * LANES] = part
    whole = [side[c] for c in range(5)]
    keep_start_powers(rhs - apply_faces(guess, whole), whole, rows, start_powers)
    for power in range(DEPTH):
        first, last = DEPTH + 1 + power, DEPTH + rows - 1 - power
        unroll = (last - first) // (2 if power < 2 else 1)

        def some_rows(i, carry, power=power, first=first, unroll=unroll):
            for u in range(unroll):
                power_rows(powers, faces, power, first + i * unroll + u, vectors)
            return carry

        lax.fori_loop(0, (last - first) // unroll, some_rows, 0)
    middle = range(DEPTH, rows - DEPTH)
    batches = [middle[at : at + DEPTH] for at in range(0, len(middle), DEPTH)]
    sums[...] = products(powers, start_powers, batches, rows)


def outer_kernel(
    inside, basis_in, powers_in, sums, sides, mask,
    from_n, from_s, from_e, from_w, corner_n, corner_s,
    copies, basis_ext, powers, side_ext, fields_ext, faces, start_powers,
):
    del basis_in, powers_in
    rows, cols = mask.shape
    wide = cols + LANES
    tall = rows + 2 * DEPTH
    tiles = cols // LANES
    vectors = basis_ext.shape[1] // tall
    halo_e = jnp.concatenate([corner_n[:DEPTH, :], corner_s[rows - DEPTH : rows, :]], axis=0)
    halo_w = [corner_n[rows : rows + DEPTH, :], corner_s[2 * rows - DEPTH :, :]]
    halo_w = jnp.concatenate(halo_w, axis=0)
    strip_e = jnp.concatenate([from_e[...], halo_e], axis=0)
    strip_w = jnp.concatenate([from_w[...], halo_w], axis=0)

    for k in range(vectors):
        at, to = DEPTH * k, tall * k + rows
        for tile in range(tiles):
            part = pl.ds(tile * LANES, LANES)
            both = [from_n[pl.ds(at, DEPTH), part], from_s[pl.ds(at, DEPTH), part]]
            basis_ext[tile, pl.ds(to, 2 * DEPTH), :] = jnp.concatenate(both, axis=0)
        basis_ext[tiles, pl.ds(to, 2 * DEPTH), :] = edges(k, halo_e, halo_w)
    own = (sides.at[0], sides.at[1], mask, sides.at[2], sides.at[3], sides.at[4])
    for f, ref in enumerate(own):
        at = DEPTH * (vectors + f)
        fields_ext[f, :rows, :cols] = ref[...].astype(jnp.float32)
        fields_ext[f, rows : rows + DEPTH, :cols] = from_n[pl.ds(at, DEPTH), :]
        fields_ext[f, rows + DEPTH :, :cols] = from_s[pl.ds(at, DEPTH), :]
        fields_ext[f, :, cols:] = edges(vectors + f, strip_e, strip_w)
    wet_halo = fields_ext[2, rows:, :] * jnp.concatenate([inside[...]] * (wide // LANES), axis=1)
    wet = jnp.concatenate([fields_ext[2, :rows, :], wet_halo], axis=0)
    for c, values in enumerate(faces_of(wet, fields_ext[3], fields_ext[4], fields_ext[5])):
        side_ext[c] = values

    for q in range(tall):
        ring_row = (q - DEPTH) % tall
        if q <= 2 * DEPTH or q >= rows - 2:
            spread_faces(side_ext, faces, q, ring_row)
        if ring_row >= rows:
            for tile in range(tiles + 1):
                part = basis_ext[tile, pl.ds(ring_row, vectors, stride=tall), :]
                powers[q, :vectors, tile * LANES : (tile + 1) * LANES] = part
    whole = [side_ext[c] for c in range(5)]
    start = fields_ext[1] - apply_faces(fields_ext[0], whole)
    side_ext[5] = start
    keep_start_powers(start, whole, rows, start_powers)
    for power in range(DEPTH):
        for u in range(DEPTH):
            power_rows(powers, faces, power, 1 + power + u, vectors)
            power_rows(powers, faces, power, tall - 2 - power - u, vectors)
    ends = [range(DEPTH), range(rows - DEPTH, rows)]
    both = products(powers, start_powers, ends, rows) + sums[...]
    base = (ITERS + 2) * vectors
    count = base + 8
    full = both[:count] + both[count:] + both[count:].T
    full = jnp.concatenate([full, jnp.zeros((count, LANES - count), jnp.float32)], axis=1)
    at = lax.broadcasted_iota(jnp.int32, (vectors, LANES), 1)
    slabs = [full[a * vectors : (a + 1) * vectors, :] for a in range(4)]
    tail = jnp.concatenate([full[base:, :], jnp.zeros((vectors - 8, LANES), jnp.float32)], axis=0)
    out = jnp.zeros((vectors, LANES), jnp.float32)

    def move(out, v, first, width, target):
        moved = pltpu.roll(v, (target - first) % LANES, 1)
        return jnp.where((at >= target) & (at < target + width), moved, out)

    out = move(out, slabs[0], vectors, vectors, 0)
    out = move(out, slabs[1], vectors, 2 * vectors, vectors)
    out = move(out, slabs[2], 2 * vectors, 2 * vectors, 3 * vectors)
    out = move(out, slabs[3], 3 * vectors, 2 * vectors, 5 * vectors)
    sub = lax.broadcasted_iota(jnp.int32, (vectors, LANES), 0)
    inner_lane = at % vectors
    diagonals = jnp.sum(jnp.where(inner_lane == sub, out, 0.0), axis=0, keepdims=True)
    shared = jnp.where(inner_lane >= sub, out, roll_lanes(out, -vectors))
    merged = out
    for t in range(1, 4):
        merged = move(merged, shared, (2 * t - 1) * vectors, vectors, t * vectors)
    half = vectors // 2
    folded = jnp.where(at[:half] < LANES // 2, merged[:half], roll_lanes(merged[half:], LANES // 2))
    first_lane = at[:1]
    with_start = jnp.zeros((1, LANES), jnp.float32)
    last_line = jnp.where(first_lane < 7 * vectors, diagonals, 0.0)
    for a in range(4):
        line = tail[a : a + 1]
        to, width = 2 * a * vectors, (1 if a == 3 else 2) * vectors
        moved = roll_lanes(line, to - a * vectors)
        with_start = jnp.where((first_lane >= to) & (first_lane < to + width), moved, with_start)
        if a < ITERS:
            to = 7 * vectors + 2 * a
            moved = roll_lanes(line, to - (base + a))
            last_line = jnp.where((first_lane >= to) & (first_lane < to + 2), moved, last_line)
    pieces = [folded[2 * i : 2 * i + 2] for i in range(half // 2)]
    pieces.append(jnp.concatenate([with_start, last_line], axis=0))
    packed = jnp.concatenate(pieces, axis=1)

    def one_copy(device, carry):
        copies[device] = packed
        return carry

    lax.fori_loop(0, copies.shape[0], one_copy, 0, unroll=8)


def finish_kernel(parts, sides, basis_ext, side_ext, solution, residual, spread):
    _, tall, wide = side_ext.shape
    _, rows, cols = sides.shape
    vectors = basis_ext.shape[1] // tall
    free = 7 * vectors
    several = 8

    def add_parts(i, sums):
        return tuple(sums[n] + parts[i * several + n] for n in range(several))

    nothing = (jnp.zeros(parts.shape[1:], jnp.float32),) * several
    sums = list(lax.fori_loop(0, parts.shape[0] // several, add_parts, nothing, unroll=2))
    while len(sums) > 1:
        sums = [sums[i] + sums[i + 1] for i in range(0, len(sums), 2)]
    total = sums[0]
    lane = lax.broadcasted_iota(jnp.int32, (vectors, LANES), 1)
    sub = lax.broadcasted_iota(jnp.int32, (vectors, LANES), 0)
    count = vectors // 4
    folded = jnp.concatenate([total[:, i * LANES : (i + 1) * LANES] for i in range(count)], axis=0)
    with_start = total[:1, count * LANES :]
    last_line = total[1:, count * LANES :]
    merged = jnp.concatenate([folded, roll_lanes(folded, LANES // 2)], axis=0)
    turned = jnp.concatenate([merged] * (LANES // vectors), axis=0).T
    columns_of = jnp.broadcast_to(with_start, (LANES, LANES)).T
    inner_lane = lane % vectors
    table = jnp.where(lane < vectors, merged, 0.0)
    for t in range(1, 4):
        flipped = turned[t * vectors : (t + 1) * vectors]
        upper = jnp.where(inner_lane >= sub, merged, flipped)
        lower = jnp.where(inner_lane < sub, merged, flipped)
        for values, block in ((upper, 2 * t - 1), (lower, 2 * t)):
            moved = roll_lanes(values, (block - t) * vectors)
            table = jnp.where(lane // vectors == block, moved, table)
    even_block = (lane // vectors) % 2 == 0
    fix = (inner_lane == sub) & even_block & (lane >= vectors) & (lane < free)
    table = jnp.where(fix, last_line, table)
    for i in range(7):
        table = jnp.where(lane == free + i, columns_of[i * vectors : (i + 1) * vectors], table)
    total = table
    columns = [jnp.broadcast_to(total[:, i : i + 1], total.shape) for i in range(vectors)]

    def row_of(values, i):
        return jnp.broadcast_to(values[i : i + 1, :], values.shape)

    for i in range(vectors):
        column = columns[i]
        inverse = 1.0 / row_of(column, i)

        def eliminate(values):
            pivot_row = row_of(values, i) * inverse
            return jnp.where(sub == i, pivot_row, values - column * pivot_row)

        columns[i + 1 :] = [eliminate(values) for values in columns[i + 1 :]]
        table = eliminate(table)
    own_lane = (lane % vectors) == sub
    z = [-table[:, free : free + 1]]
    sums = jnp.zeros((vectors, LANES), jnp.float32)
    history = jnp.zeros((1, LANES), jnp.float32)
    lane_row = lane[:1, :]
    for j in range(2 * ITERS):
        newest = jnp.sum(jnp.where(own_lane, z[j], 0.0), axis=0, keepdims=True)
        history = pltpu.roll(history, vectors, 1)
        history = jnp.where((lane_row >= vectors) & (lane_row < 2 * vectors), newest, history)
        terms = (lane >= vectors) & (lane < (j + 2) * vectors)
        weights = jnp.where(terms, history, jnp.where(lane == free + 1 + j, 1.0, 0.0))
        z.append(-jnp.sum(table * weights, axis=1, keepdims=True))
    for j in range(2 * ITERS + 1):
        sums = sums + pltpu.roll(jnp.where(lane >= free, total, 0.0) * z[j], j, 1)
    picked = jnp.where((lane > free) & (lane < free + 7), sums, 0.0)
    moment_row = jnp.sum(picked, axis=0, keepdims=True)
    moment_row += jnp.where(lane_row > free, roll_lanes(last_line, 1), 0.0)
    mu = [moment_row[:, free + 1 + k : free + 2 + k] for k in range(2 * ITERS)]
    for i in range(ITERS + 1):
        spread[i] = jnp.broadcast_to(z[i], (vectors, LANES))

    nil = jnp.zeros((1, 1), jnp.float32)
    rho = [nil + 1.0] + [nil] * ITERS
    gamma = [nil] * (ITERS + 1)
    delta = [nil] * ITERS
    curv = nil
    prev = nil
    for j in range(ITERS):
        norm = nil
        image = nil
        for a in range(j + 1):
            for b in range(j + 1):
                pair = rho[a] * rho[b]
                norm += pair * mu[a + b]
                image += pair * (mu[a + b + 1] + SHIFT * mu[a + b])
        if j == 0:
            gamma = list(rho)
            curv = image
        else:
            ratio = norm / prev
            gamma = [rho[i] + ratio * gamma[i] for i in range(ITERS + 1)]
            curv = image - ratio * ratio * curv
        step = norm / curv
        delta = [delta[i] + step * gamma[i] for i in range(ITERS)]
        below = [nil] + gamma[:ITERS]
        rho = [rho[i] - step * (SHIFT * gamma[i] + below[i]) for i in range(ITERS + 1)]
        prev = norm

    along = [[] for _ in range(ITERS + 1)]
    for tile in range(wide // LANES):
        acc = [jnp.zeros((tall, LANES), jnp.float32) for _ in range(ITERS + 1)]
        for k in range(vectors):
            w = basis_ext[tile, pl.ds(tall * k, tall), :]
            for i in range(ITERS + 1):
                acc[i] = acc[i] + w * spread[i, pl.ds(k, 1), :]
        for i in range(ITERS + 1):
            along[i].append(acc[i])
    along = [jnp.concatenate(pieces, axis=1) for pieces in along]
    faces = [side_ext[c] for c in range(5)]
    v = side_ext[5] + apply_faces(along[0], faces)
    x = sides[0] - along[0][:rows, :cols]
    r = rho[0] * v[:rows, :cols]
    for i in range(ITERS):
        x = x + delta[i] * (v + along[i + 1])[:rows, :cols]
        v = apply_faces(v, faces, SHIFT) + apply_faces(along[i + 1], faces)
        r = r + rho[i + 1] * v[:rows, :cols]
    solution[...] = x
    residual[...] = r


def call(kernel, out_shape, spaces, inputs, scratch=(), flops=10**6, aliases={}):
    return pl.pallas_call(
        kernel,
        out_shape=out_shape,
        in_specs=[pl.BlockSpec(memory_space=space) for space in spaces],
        out_specs=[pl.BlockSpec(memory_space=pltpu.VMEM)] * len(out_shape),
        scratch_shapes=scratch,
        input_output_aliases=aliases,
        cost_estimate=pl.CostEstimate(flops=flops, bytes_accessed=10**6, transcendentals=0),
        compiler_params=pltpu.CompilerParams(vmem_limit_bytes=24 * 1024 * 1024),
    )(*inputs)


def f32(*shape):
    return jax.ShapeDtypeStruct(shape, jnp.float32)


def shards(right_side, first_guess, cell_mask, cond_east, cond_north, surface, recycled):
    vectors, rows, cols = recycled.shape
    n_lat, n_lon = lax.axis_size("lat"), lax.axis_size("lon")
    devices = n_lat * n_lon
    fields = vectors + 6
    tall, wide = rows + 2 * DEPTH, cols + LANES
    tiles = cols // LANES
    own = (recycled, first_guess, right_side, cell_mask, cond_east, cond_north, surface)
    band, strip = f32(fields * DEPTH, cols), f32(rows, LANES)
    basis, sides, mask, to_n, to_s, to_e, to_w = call(
        pack_kernel,
        [f32(vectors, rows, cols), f32(5, rows, cols), jax.ShapeDtypeStruct((rows, cols), jnp.int32)]
        + [band, band, strip, strip],
        [pltpu.HBM] * 7,
        [pltpu.with_memory_space_constraint(array, pltpu.HBM) for array in own],
        scratch=[pltpu.SemaphoreType.DMA((7,))],
    )
    north, south = ring(n_lat, 1), ring(n_lat, -1)
    from_w = lax.ppermute(to_e, "lon", ring(n_lon, 1))
    from_e = lax.ppermute(to_w, "lon", ring(n_lon, -1))
    from_s = lax.ppermute(to_n, "lat", north)
    from_n = lax.ppermute(to_s, "lat", south)
    strips = jnp.concatenate([from_e, from_w], axis=0)
    corner_s = lax.ppermute(strips, "lat", north)
    corner_n = lax.ppermute(strips, "lat", south)
    here = lax.axis_index("lat")
    inside = jnp.stack([here < n_lat - 1, here > 0]).astype(jnp.float32)
    inside = jnp.broadcast_to(inside[:, None, None], (2, DEPTH, LANES)).reshape(-1, LANES)
    count = (ITERS + 2) * vectors
    powers = f32(tall, count, wide)
    basis_ext = f32(tiles + 1, vectors * tall, LANES)
    faces = pltpu.VMEM((5, tall, 8, wide), jnp.float32)
    start_powers = pltpu.VMEM((tiles, 8 * rows, LANES), jnp.float32)
    powers, basis_ext, sums = call(
        inner_kernel,
        [powers, basis_ext, f32(2 * (count + 8), count + 8)],
        [pltpu.VMEM] * 5,
        (basis, sides, mask, from_e, from_w),
        scratch=[pltpu.VMEM((5, rows, wide), jnp.float32), faces, start_powers],
        flops=10**9,
    )
    copies, basis_ext, _, side_ext = call(
        outer_kernel,
        [f32(devices, 2, (vectors // 4 + 1) * LANES), basis_ext, powers, f32(6, tall, wide)],
        [pltpu.VMEM] * 12,
        (inside, basis_ext, powers, sums, sides, mask)
        + (from_n, from_s, from_e, from_w, corner_n, corner_s),
        scratch=[pltpu.VMEM((6, tall, wide), jnp.float32), faces, start_powers],
        aliases={1: 1, 2: 2},
    )
    parts = lax.all_to_all(copies, ("lat", "lon"), 0, 0)
    return call(
        finish_kernel,
        [f32(rows, cols), f32(rows, cols)],
        [pltpu.VMEM] * 4,
        (parts, sides, basis_ext, side_ext),
        scratch=[pltpu.VMEM((ITERS + 1, vectors, LANES), jnp.float32)],
    )


def solution(mesh):
    block = P("lat", "lon")
    return jax.shard_map(
        shards,
        mesh=mesh,
        in_specs=(block,) * 6 + (P(None, "lat", "lon"),),
        out_specs=(block, block),
        check_vma=False,
    )
```

```python
import jax
import jax.numpy as jnp
from jax import lax
from jax.experimental import pallas as pl
from jax.experimental.pallas import tpu as pltpu
from jax.sharding import PartitionSpec as P

SHIFT = 5.0
ITERS = 3
DEPTH = ITERS + 1
LANES = 128


def ring(count, step):
    return [(i, (i + step) % count) for i in range(count)]


def pack_kernel(
    basis_hbm, guess_hbm, rhs_hbm, mask_hbm, east_hbm, north_hbm, surf_hbm,
    basis, sides, mask, to_n, to_s, to_e, to_w, sems,
):
    vectors, rows, cols = basis.shape
    moves = [(basis_hbm, basis), (mask_hbm, mask)]
    sources = (guess_hbm, rhs_hbm, east_hbm, north_hbm, surf_hbm)
    moves += [(source, sides.at[i]) for i, source in enumerate(sources)]
    copies = [pltpu.make_async_copy(a, b, sems.at[i]) for i, (a, b) in enumerate(moves)]
    for copy in copies:
        copy.start()
    for copy in copies:
        copy.wait()
    fields = [basis.at[k] for k in range(vectors)]
    fields += [sides.at[0], sides.at[1], mask, sides.at[2], sides.at[3], sides.at[4]]
    strip_e = jnp.zeros((rows, LANES), jnp.float32)
    strip_w = jnp.zeros((rows, LANES), jnp.float32)
    lane = lax.broadcasted_iota(jnp.int32, (rows, LANES), 1)
    for f, ref in enumerate(fields):
        at = DEPTH * f
        to_n[pl.ds(at, DEPTH), :] = ref[rows - DEPTH :, :].astype(jnp.float32)
        to_s[pl.ds(at, DEPTH), :] = ref[:DEPTH, :].astype(jnp.float32)
        here = (lane >= at) & (lane < at + DEPTH)
        last = ref[:, cols - LANES :].astype(jnp.float32)
        first = ref[:, :LANES].astype(jnp.float32)
        strip_e = jnp.where(here, pltpu.roll(last, (at + DEPTH) % LANES, 1), strip_e)
        strip_w = jnp.where(here, pltpu.roll(first, at, 1), strip_w)
    to_e[...] = strip_e
    to_w[...] = strip_w


def roll_lanes(v, by):
    return pltpu.roll(v, by % v.shape[1], 1)


def roll_rows(v, by):
    return pltpu.roll(v, by % v.shape[0], 0)


def apply_faces(v, faces, shift=0.0):
    centre, k_east, k_west, k_north, k_south = faces
    beside = k_east * roll_lanes(v, -1) + k_west * roll_lanes(v, 1)
    above = k_north * roll_rows(v, -1) + k_south * roll_rows(v, 1)
    return (centre - shift) * v - (beside + above)


def edges(f, strip_e, strip_w):
    at = DEPTH * f
    lane = lax.broadcasted_iota(jnp.int32, strip_e.shape, 1)
    edge_e = pltpu.roll(strip_e, (-at) % LANES, 1)
    edge_w = pltpu.roll(strip_w, (LANES - DEPTH - at) % LANES, 1)
    return jnp.where(lane < DEPTH, edge_e, jnp.where(lane >= LANES - DEPTH, edge_w, 0.0))


def faces_of(wet, east, north, surf):
    k_east = east * wet * roll_lanes(wet, -1)
    k_north = north * wet * roll_rows(wet, -1)
    k_west = roll_lanes(k_east, 1)
    k_south = roll_rows(k_north, 1)
    centre = surf * wet + k_east + k_west + k_north + k_south + (1.0 - wet)
    return centre, k_east, k_west, k_north, k_south


def spread_faces(side, faces, q, row):
    for c in range(4):
        line = side[c, row : row + 1, :]
        spread = jnp.broadcast_to(line, (8, line.shape[1]))
        faces[c, q] = spread
        if c == 0:
            faces[4, q] = spread - SHIFT


def power_rows(powers, faces, power, q, vectors):
    source = slice(power * vectors, (power + 1) * vectors)
    target = slice((power + 1) * vectors, (power + 2) * vectors)

    def coefficient(c, q):
        return jnp.concatenate([faces[c, q]] * (vectors // 8), axis=0)

    v = powers[q, source, :]
    beside = coefficient(1, q) * roll_lanes(v, -1) + coefficient(2, q) * roll_lanes(v, 1)
    above = coefficient(3, q) * powers[q + 1, source, :]
    above += coefficient(3, q - 1) * powers[q - 1, source, :]
    middle = coefficient(0 if power == 0 else 4, q)
    powers[q, target, :] = middle * v - (beside + above)


def keep_start_powers(v, faces, rows, start_powers):
    tiles = start_powers.shape[0]
    for power in range(ITERS + 1):
        for tile in range(tiles):
            part = v[:rows, tile * LANES : (tile + 1) * LANES]
            start_powers[tile, pl.ds(power * rows, rows), :] = part
        if power < ITERS:
            v = apply_faces(v, faces, SHIFT)
    spare = (8 - (ITERS + 1)) * rows
    start_powers[:, pl.ds((ITERS + 1) * rows, spare), :] = jnp.zeros(
        (tiles, spare, LANES), jnp.float32
    )


def products(powers, start_powers, batches, rows):
    tiles = start_powers.shape[0]
    nt = (((1,), (1,)), ((), ()))
    total = 0.0
    for batch in batches:
        x = []
        for r in batch:
            tail = [start_powers[t, pl.ds(r, 8, stride=rows), :] for t in range(tiles)]
            tail = jnp.concatenate(tail, axis=1)
            x.append(jnp.concatenate([powers[r + DEPTH, :, : tiles * LANES], tail], axis=0))
        x = jnp.concatenate(x, axis=1)
        high = x.astype(jnp.bfloat16)
        low = (x - high.astype(jnp.float32)).astype(jnp.bfloat16)
        both = jnp.concatenate([high, low], axis=0)
        total += lax.dot_general(both, both, nt, preferred_element_type=jnp.float32)
    return total


def inner_kernel(
    basis, sides, mask, from_e, from_w,
    powers, basis_ext, sums, side, faces, start_powers,
):
    vectors, rows, cols = basis.shape
    tall = rows + 2 * DEPTH
    tiles = cols // LANES
    strip_e, strip_w = from_e[...], from_w[...]
    for k in range(vectors):
        for tile in range(tiles):
            basis_ext[tile, pl.ds(tall * k, rows), :] = basis[k, :, tile * LANES : (tile + 1) * LANES]
        basis_ext[tiles, pl.ds(tall * k, rows), :] = edges(k, strip_e, strip_w)
    own = (sides[0], sides[1], mask[...].astype(jnp.float32), sides[2], sides[3], sides[4])
    guess, rhs, wet, east, north, surf = [
        jnp.concatenate([v, edges(vectors + f, strip_e, strip_w)], axis=1)
        for f, v in enumerate(own)
    ]
    for c, values in enumerate(faces_of(wet, east, north, surf)):
        side[c] = values
    for row in range(rows):
        spread_faces(side, faces, row + DEPTH, row)
        for tile in range(tiles + 1):
            part = basis_ext[tile, pl.ds(row, vectors, stride=tall), :]
            powers[row + DEPTH, :vectors, tile * LANES : (tile + 1) * LANES] = part
    whole = [side[c] for c in range(5)]
    keep_start_powers(rhs - apply_faces(guess, whole), whole, rows, start_powers)
    for power in range(DEPTH):
        first, last = DEPTH + 1 + power, DEPTH + rows - 1 - power
        unroll = (last - first) // (2 if power < 2 else 1)

        def some_rows(i, carry, power=power, first=first, unroll=unroll):
            for u in range(unroll):
                power_rows(powers, faces, power, first + i * unroll + u, vectors)
            return carry

        lax.fori_loop(0, (last - first) // unroll, some_rows, 0)
    middle = range(DEPTH, rows - DEPTH)
    batches = [middle[at : at + DEPTH] for at in range(0, len(middle), DEPTH)]
    sums[...] = products(powers, start_powers, batches, rows)


def outer_kernel(
    inside, basis_in, powers_in, sums, sides, mask,
    from_n, from_s, from_e, from_w, corner_n, corner_s,
    copies, basis_ext, powers, side_ext, fields_ext, faces, start_powers,
):
    del basis_in, powers_in
    rows, cols = mask.shape
    wide = cols + LANES
    tall = rows + 2 * DEPTH
    tiles = cols // LANES
    vectors = basis_ext.shape[1] // tall
    halo_e = jnp.concatenate([corner_n[:DEPTH, :], corner_s[rows - DEPTH : rows, :]], axis=0)
    halo_w = [corner_n[rows : rows + DEPTH, :], corner_s[2 * rows - DEPTH :, :]]
    halo_w = jnp.concatenate(halo_w, axis=0)
    strip_e = jnp.concatenate([from_e[...], halo_e], axis=0)
    strip_w = jnp.concatenate([from_w[...], halo_w], axis=0)

    for k in range(vectors):
        at, to = DEPTH * k, tall * k + rows
        for tile in range(tiles):
            part = pl.ds(tile * LANES, LANES)
            both = [from_n[pl.ds(at, DEPTH), part], from_s[pl.ds(at, DEPTH), part]]
            basis_ext[tile, pl.ds(to, 2 * DEPTH), :] = jnp.concatenate(both, axis=0)
        basis_ext[tiles, pl.ds(to, 2 * DEPTH), :] = edges(k, halo_e, halo_w)
    own = (sides.at[0], sides.at[1], mask, sides.at[2], sides.at[3], sides.at[4])
    for f, ref in enumerate(own):
        at = DEPTH * (vectors + f)
        fields_ext[f, :rows, :cols] = ref[...].astype(jnp.float32)
        fields_ext[f, rows : rows + DEPTH, :cols] = from_n[pl.ds(at, DEPTH), :]
        fields_ext[f, rows + DEPTH :, :cols] = from_s[pl.ds(at, DEPTH), :]
        fields_ext[f, :, cols:] = edges(vectors + f, strip_e, strip_w)
    wet_halo = fields_ext[2, rows:, :] * jnp.concatenate([inside[...]] * (wide // LANES), axis=1)
    wet = jnp.concatenate([fields_ext[2, :rows, :], wet_halo], axis=0)
    for c, values in enumerate(faces_of(wet, fields_ext[3], fields_ext[4], fields_ext[5])):
        side_ext[c] = values

    for q in range(tall):
        ring_row = (q - DEPTH) % tall
        if q <= 2 * DEPTH or q >= rows - 2:
            spread_faces(side_ext, faces, q, ring_row)
        if ring_row >= rows:
            for tile in range(tiles + 1):
                part = basis_ext[tile, pl.ds(ring_row, vectors, stride=tall), :]
                powers[q, :vectors, tile * LANES : (tile + 1) * LANES] = part
    whole = [side_ext[c] for c in range(5)]
    start = fields_ext[1] - apply_faces(fields_ext[0], whole)
    side_ext[5] = start
    keep_start_powers(start, whole, rows, start_powers)
    for power in range(DEPTH):
        for u in range(DEPTH):
            power_rows(powers, faces, power, 1 + power + u, vectors)
            power_rows(powers, faces, power, tall - 2 - power - u, vectors)
    ends = [range(DEPTH), range(rows - DEPTH, rows)]
    both = products(powers, start_powers, ends, rows) + sums[...]
    base = (ITERS + 2) * vectors
    count = base + 8
    full = both[:count] + both[count:]
    full = full[:, :count] + full[:, count:]
    full = jnp.concatenate([full, jnp.zeros((count, LANES - count), jnp.float32)], axis=1)
    at = lax.broadcasted_iota(jnp.int32, (vectors, LANES), 1)
    slabs = [full[a * vectors : (a + 1) * vectors, :] for a in range(4)]
    tail = jnp.concatenate([full[base:, :], jnp.zeros((vectors - 8, LANES), jnp.float32)], axis=0)
    out = jnp.zeros((vectors, LANES), jnp.float32)

    def move(out, v, first, width, target):
        moved = pltpu.roll(v, (target - first) % LANES, 1)
        return jnp.where((at >= target) & (at < target + width), moved, out)

    out = move(out, slabs[0], vectors, vectors, 0)
    out = move(out, slabs[1], vectors, 2 * vectors, vectors)
    out = move(out, slabs[2], 2 * vectors, 2 * vectors, 3 * vectors)
    out = move(out, slabs[3], 3 * vectors, 2 * vectors, 5 * vectors)
    sub = lax.broadcasted_iota(jnp.int32, (vectors, LANES), 0)
    inner_lane = at % vectors
    diagonals = jnp.sum(jnp.where(inner_lane == sub, out, 0.0), axis=0, keepdims=True)
    shared = jnp.where(inner_lane >= sub, out, roll_lanes(out, -vectors))
    merged = out
    for t in range(1, 4):
        merged = move(merged, shared, (2 * t - 1) * vectors, vectors, t * vectors)
    half = vectors // 2
    folded = jnp.where(at[:half] < LANES // 2, merged[:half], roll_lanes(merged[half:], LANES // 2))
    first_lane = at[:1]
    with_start = jnp.zeros((1, LANES), jnp.float32)
    last_line = jnp.where(first_lane < 7 * vectors, diagonals, 0.0)
    for a in range(4):
        line = tail[a : a + 1]
        to, width = 2 * a * vectors, (1 if a == 3 else 2) * vectors
        moved = roll_lanes(line, to - a * vectors)
        with_start = jnp.where((first_lane >= to) & (first_lane < to + width), moved, with_start)
        if a < ITERS:
            to = 7 * vectors + 2 * a
            moved = roll_lanes(line, to - (base + a))
            last_line = jnp.where((first_lane >= to) & (first_lane < to + 2), moved, last_line)
    pieces = [folded[2 * i : 2 * i + 2] for i in range(half // 2)]
    pieces.append(jnp.concatenate([with_start, last_line], axis=0))
    packed = jnp.concatenate(pieces, axis=1)

    def one_copy(device, carry):
        copies[device] = packed
        return carry

    lax.fori_loop(0, copies.shape[0], one_copy, 0, unroll=8)


def finish_kernel(parts, sides, basis_ext, side_ext, solution, residual, spread):
    _, tall, wide = side_ext.shape
    _, rows, cols = sides.shape
    vectors = basis_ext.shape[1] // tall
    free = 7 * vectors
    several = 8

    def add_parts(i, sums):
        return tuple(sums[n] + parts[i * several + n] for n in range(several))

    nothing = (jnp.zeros(parts.shape[1:], jnp.float32),) * several
    sums = list(lax.fori_loop(0, parts.shape[0] // several, add_parts, nothing, unroll=2))
    while len(sums) > 1:
        sums = [sums[i] + sums[i + 1] for i in range(0, len(sums), 2)]
    total = sums[0]
    lane = lax.broadcasted_iota(jnp.int32, (vectors, LANES), 1)
    sub = lax.broadcasted_iota(jnp.int32, (vectors, LANES), 0)
    count = vectors // 4
    folded = jnp.concatenate([total[:, i * LANES : (i + 1) * LANES] for i in range(count)], axis=0)
    with_start = total[:1, count * LANES :]
    last_line = total[1:, count * LANES :]
    merged = jnp.concatenate([folded, roll_lanes(folded, LANES // 2)], axis=0)
    turned = jnp.concatenate([merged] * (LANES // vectors), axis=0).T
    columns_of = jnp.broadcast_to(with_start, (LANES, LANES)).T
    inner_lane = lane % vectors
    table = jnp.where(lane < vectors, merged, 0.0)
    for t in range(1, 4):
        flipped = turned[t * vectors : (t + 1) * vectors]
        upper = jnp.where(inner_lane >= sub, merged, flipped)
        lower = jnp.where(inner_lane < sub, merged, flipped)
        for values, block in ((upper, 2 * t - 1), (lower, 2 * t)):
            moved = roll_lanes(values, (block - t) * vectors)
            table = jnp.where(lane // vectors == block, moved, table)
    even_block = (lane // vectors) % 2 == 0
    fix = (inner_lane == sub) & even_block & (lane >= vectors) & (lane < free)
    table = jnp.where(fix, last_line, table)
    for i in range(7):
        table = jnp.where(lane == free + i, columns_of[i * vectors : (i + 1) * vectors], table)
    total = table
    columns = [jnp.broadcast_to(total[:, i : i + 1], total.shape) for i in range(vectors)]

    def row_of(values, i):
        return jnp.broadcast_to(values[i : i + 1, :], values.shape)

    for i in range(vectors):
        column = columns[i]
        inverse = 1.0 / row_of(column, i)

        def eliminate(values):
            pivot_row = row_of(values, i) * inverse
            return jnp.where(sub == i, pivot_row, values - column * pivot_row)

        columns[i + 1 :] = [eliminate(values) for values in columns[i + 1 :]]
        table = eliminate(table)
    own_lane = (lane % vectors) == sub
    z = [-table[:, free : free + 1]]
    sums = jnp.zeros((vectors, LANES), jnp.float32)
    history = jnp.zeros((1, LANES), jnp.float32)
    lane_row = lane[:1, :]
    for j in range(2 * ITERS):
        newest = jnp.sum(jnp.where(own_lane, z[j], 0.0), axis=0, keepdims=True)
        history = pltpu.roll(history, vectors, 1)
        history = jnp.where((lane_row >= vectors) & (lane_row < 2 * vectors), newest, history)
        terms = (lane >= vectors) & (lane < (j + 2) * vectors)
        weights = jnp.where(terms, history, jnp.where(lane == free + 1 + j, 1.0, 0.0))
        z.append(-jnp.sum(table * weights, axis=1, keepdims=True))
    for j in range(2 * ITERS + 1):
        sums = sums + pltpu.roll(jnp.where(lane >= free, total, 0.0) * z[j], j, 1)
    picked = jnp.where((lane > free) & (lane < free + 7), sums, 0.0)
    moment_row = jnp.sum(picked, axis=0, keepdims=True)
    moment_row += jnp.where(lane_row > free, roll_lanes(last_line, 1), 0.0)
    mu = [moment_row[:, free + 1 + k : free + 2 + k] for k in range(2 * ITERS)]
    for i in range(ITERS + 1):
        spread[i] = jnp.broadcast_to(z[i], (vectors, LANES))

    nil = jnp.zeros((1, 1), jnp.float32)
    rho = [nil + 1.0] + [nil] * ITERS
    gamma = [nil] * (ITERS + 1)
    delta = [nil] * ITERS
    curv = nil
    prev = nil
    for j in range(ITERS):
        norm = nil
        image = nil
        for a in range(j + 1):
            for b in range(j + 1):
                pair = rho[a] * rho[b]
                norm += pair * mu[a + b]
                image += pair * (mu[a + b + 1] + SHIFT * mu[a + b])
        if j == 0:
            gamma = list(rho)
            curv = image
        else:
            ratio = norm / prev
            gamma = [rho[i] + ratio * gamma[i] for i in range(ITERS + 1)]
            curv = image - ratio * ratio * curv
        step = norm / curv
        delta = [delta[i] + step * gamma[i] for i in range(ITERS)]
        below = [nil] + gamma[:ITERS]
        rho = [rho[i] - step * (SHIFT * gamma[i] + below[i]) for i in range(ITERS + 1)]
        prev = norm

    along = [[] for _ in range(ITERS + 1)]
    for tile in range(wide // LANES):
        acc = [jnp.zeros((tall, LANES), jnp.float32) for _ in range(ITERS + 1)]
        for k in range(vectors):
            w = basis_ext[tile, pl.ds(tall * k, tall), :]
            for i in range(ITERS + 1):
                acc[i] = acc[i] + w * spread[i, pl.ds(k, 1), :]
        for i in range(ITERS + 1):
            along[i].append(acc[i])
    along = [jnp.concatenate(pieces, axis=1) for pieces in along]
    faces = [side_ext[c] for c in range(5)]
    v = side_ext[5] + apply_faces(along[0], faces)
    x = sides[0] - along[0][:rows, :cols]
    r = rho[0] * v[:rows, :cols]
    for i in range(ITERS):
        x = x + delta[i] * (v + along[i + 1])[:rows, :cols]
        v = apply_faces(v, faces, SHIFT) + apply_faces(along[i + 1], faces)
        r = r + rho[i + 1] * v[:rows, :cols]
    solution[...] = x
    residual[...] = r


def call(kernel, out_shape, spaces, inputs, scratch=(), flops=10**6, aliases={}):
    return pl.pallas_call(
        kernel,
        out_shape=out_shape,
        in_specs=[pl.BlockSpec(memory_space=space) for space in spaces],
        out_specs=[pl.BlockSpec(memory_space=pltpu.VMEM)] * len(out_shape),
        scratch_shapes=scratch,
        input_output_aliases=aliases,
        cost_estimate=pl.CostEstimate(flops=flops, bytes_accessed=10**6, transcendentals=0),
        compiler_params=pltpu.CompilerParams(vmem_limit_bytes=24 * 1024 * 1024),
    )(*inputs)


def f32(*shape):
    return jax.ShapeDtypeStruct(shape, jnp.float32)


def shards(right_side, first_guess, cell_mask, cond_east, cond_north, surface, recycled):
    vectors, rows, cols = recycled.shape
    n_lat, n_lon = lax.axis_size("lat"), lax.axis_size("lon")
    devices = n_lat * n_lon
    fields = vectors + 6
    tall, wide = rows + 2 * DEPTH, cols + LANES
    tiles = cols // LANES
    own = (recycled, first_guess, right_side, cell_mask, cond_east, cond_north, surface)
    band, strip = f32(fields * DEPTH, cols), f32(rows, LANES)
    basis, sides, mask, to_n, to_s, to_e, to_w = call(
        pack_kernel,
        [f32(vectors, rows, cols), f32(5, rows, cols), jax.ShapeDtypeStruct((rows, cols), jnp.int32)]
        + [band, band, strip, strip],
        [pltpu.HBM] * 7,
        [pltpu.with_memory_space_constraint(array, pltpu.HBM) for array in own],
        scratch=[pltpu.SemaphoreType.DMA((7,))],
    )
    north, south = ring(n_lat, 1), ring(n_lat, -1)
    from_w = lax.ppermute(to_e, "lon", ring(n_lon, 1))
    from_e = lax.ppermute(to_w, "lon", ring(n_lon, -1))
    from_s = lax.ppermute(to_n, "lat", north)
    from_n = lax.ppermute(to_s, "lat", south)
    strips = jnp.concatenate([from_e, from_w], axis=0)
    corner_s = lax.ppermute(strips, "lat", north)
    corner_n = lax.ppermute(strips, "lat", south)
    here = lax.axis_index("lat")
    inside = jnp.stack([here < n_lat - 1, here > 0]).astype(jnp.float32)
    inside = jnp.broadcast_to(inside[:, None, None], (2, DEPTH, LANES)).reshape(-1, LANES)
    count = (ITERS + 2) * vectors
    powers = f32(tall, count, wide)
    basis_ext = f32(tiles + 1, vectors * tall, LANES)
    faces = pltpu.VMEM((5, tall, 8, wide), jnp.float32)
    start_powers = pltpu.VMEM((tiles, 8 * rows, LANES), jnp.float32)
    powers, basis_ext, sums = call(
        inner_kernel,
        [powers, basis_ext, f32(2 * (count + 8), 2 * (count + 8))],
        [pltpu.VMEM] * 5,
        (basis, sides, mask, from_e, from_w),
        scratch=[pltpu.VMEM((5, rows, wide), jnp.float32), faces, start_powers],
        flops=10**9,
    )
    copies, basis_ext, _, side_ext = call(
        outer_kernel,
        [f32(devices, 2, (vectors // 4 + 1) * LANES), basis_ext, powers, f32(6, tall, wide)],
        [pltpu.VMEM] * 12,
        (inside, basis_ext, powers, sums, sides, mask)
        + (from_n, from_s, from_e, from_w, corner_n, corner_s),
        scratch=[pltpu.VMEM((6, tall, wide), jnp.float32), faces, start_powers],
        aliases={1: 1, 2: 2},
    )
    parts = lax.all_to_all(copies, ("lat", "lon"), 0, 0)
    return call(
        finish_kernel,
        [f32(rows, cols), f32(rows, cols)],
        [pltpu.VMEM] * 4,
        (parts, sides, basis_ext, side_ext),
        scratch=[pltpu.VMEM((ITERS + 1, vectors, LANES), jnp.float32)],
    )


def solution(mesh):
    block = P("lat", "lon")
    return jax.shard_map(
        shards,
        mesh=mesh,
        in_specs=(block,) * 6 + (P(None, "lat", "lon"),),
        out_specs=(block, block),
        check_vma=False,
    )
```
